128 devices in a mesh: row: 16 (over z, y), col: 8 (over x, core).
Axes of the slice: x: 4, y: 4, z: 4, core: 2. Of those that a mesh axis runs over, the one named last changes fastest.
Arguments:
- grads: float32 [64, 20, 3, 16384], P(None, None, None, ('row', 'col')), may hold values from -6 to 6
- weights: float32 [64, 16384], P(None, ('row', 'col')), may hold values from 0.005 to 0.05
- counts: int32 [16384], P(('row', 'col')), may hold values from 1 to 8
- lame_first: float32 [16384], P(('row', 'col')), may hold values from 0.5 to 2
- shear: float32 [16384], P(('row', 'col')), may hold values from 0.5 to 2
- dest_owner: int32 [16384, 1], P(('row', 'col')), may hold values from 0 to 127; in each aligned block of 128 rows (0 to 127, 128 to 255, ...) at most 2 rows name the same one
- dest_slot: int32 [16384], P(('row', 'col')), may hold values from 0 to 127
Outputs:
- assembled: float32 [60, 60, 16384], P(None, None, ('row', 'col'))
The draws below stay inside these ranges and needn't reach their ends.
Inputs may be any that keep to these rules, and one draw needn't show every extreme that they name: `dest_owner`: among the elements of one device, at most 2 have the same owner; in some device exactly 2 do.
All inputs are finite; a program needn't handle non-finite values.
Results may differ from the reference program's by a relative error of at most 0.0001.
Values sent between devices are 32-bit elements; how exact they have to be, the bound alone decides.
A program may use at most 64 MiB of HBM per device.

```python
import math
import jax
import jax.numpy as jnp
import numpy as np
from jax import lax

NF = 20
NDOF = 60
GP = 8
SUBMAX = 8
Q = 64
E_DEV = 128
SLOTS_DEV = 128
ELEMS = 16384
SLOTS = 16384
CAP = 2
N_ROW = 16
N_COL = 8
DEVICES = 128


def plant(entries, rng, low, high):
    longest = entries.shape.index(max(entries.shape))
    spots = []
    for shift in (0, 1):
        where = [jax.random.randint(jax.random.fold_in(rng, axis), (), 0, length) for axis, length in enumerate(entries.shape)]
        where[longest] = (where[longest] + shift) % entries.shape[longest]
        spots.append(tuple(where))
    return entries.at[spots[0]].set(low).at[spots[1]].set(high)


def steps_of(stream_key, dims, split, smallest, high):
    def one(position, shards_of):
        draws = jax.random.uniform(jax.random.fold_in(jax.random.fold_in(stream_key, 6), position), (shards_of,), jnp.float32, smallest / len(split), high / len(split))
        return jnp.repeat(jnp.exp(draws), dims[position] // shards_of).reshape((-1,) + (1,) * (len(dims) - position - 1))

    gain = one(*split[0])
    for cut in split[1:]:
        gain = gain * one(*cut)
    return gain


def assign_block(rng, own, number, rows, number_of, top, limit, skew):
    order = jax.random.permutation(rng, number_of)
    crowded, usual = load_shares(number_of, rows * top, limit, skew, True), load_shares(number_of, rows * top, limit, skew, False)
    places = jnp.arange(number_of)

    def named(lengths, turn):
        used = int((lengths > 0).sum())
        fixed = max(1, used // 4)
        moved = fixed + (places - fixed + turn * (used - fixed)) % max(1, number_of - fixed)
        return jnp.zeros((number_of,), jnp.int32).at[order[jnp.where(places < fixed, places, moved)]].set(jnp.asarray(lengths, jnp.int32))

    lengths = jnp.where(number % 4 == 0, named(crowded, number // 4), named(usual, number - number // 4 - 1))
    mixed = jax.random.permutation(jax.random.fold_in(own, 3), number_of)
    giver, sink = mixed[0:number_of // 2 * 2:2], mixed[1:number_of // 2 * 2:2]
    margin = jnp.minimum(lengths[giver] - 1, limit - lengths[sink]) // 2
    margin = jnp.where((giver == order[0]) | (sink == order[0]) | (lengths[sink] == 0), 0, jnp.maximum(margin, 0))
    moved = jax.random.randint(jax.random.fold_in(own, 4), (number_of // 2,), 0, 1 << 20) % (margin + 1)
    lengths = lengths.at[giver].add(-moved).at[sink].add(moved)
    members = jnp.searchsorted(jnp.cumsum(lengths), jnp.arange(rows * top), side="right").astype(jnp.int32)
    listing = members.reshape(top, rows).T
    listing = listing[jax.random.permutation(jax.random.fold_in(own, 1), rows)]
    turn = jax.random.randint(jax.random.fold_in(own, 2), (rows, 1), 0, top)
    return jnp.take_along_axis(listing, (jnp.arange(top)[None, :] + turn) % top, axis=1)


def load_shares(number_of, total, reach, lean, full):
    weights = [(1 << 20) // math.isqrt(rank ** lean) + 1 for rank in range(1, number_of + 1)]
    largest = reach if full else min(reach, max(-(-total // number_of), total * weights[0] // sum(weights)))
    least = 1 if total - largest >= number_of - 1 else 0
    given, surplus = [largest] + [least] * (number_of - 1), total - largest - least * (number_of - 1)
    while surplus > 0:
        free = [i for i in range(1, number_of) if given[i] < largest] or [i for i in range(1, number_of) if given[i] < reach]
        pool, budget = sum([weights[i] for i in free]), surplus
        for i in free:
            addition = min(reach - given[i], max(1, budget * weights[i] // pool), surplus)
            given[i] = given[i] + addition
            surplus = surplus - addition
    return np.array(given)


def normal_values(rng, shape, scale, limit, shards=(), held_as=jnp.bfloat16):
    values = scale * jax.random.normal(rng, shape, jnp.float32)
    if shards:
        values = values * steps_of(rng, shape, shards, -0.22, 0.18)
    return jnp.clip(values, -limit, limit).astype(held_as)


def setup_inputs(seed: int = 0) -> dict:
    key_of = jax.random.split(jax.random.key(seed), 8)
    grads = normal_values(key_of[0], (Q, NF, 3, ELEMS), 1.0, 6.0, ((3, 128),), jnp.float32)
    weights = jnp.clip(jnp.exp(math.log(0.05) - 2.3025851 * jax.random.uniform(key_of[1], (Q, ELEMS), jnp.float32) ** steps_of(key_of[1], (Q, ELEMS), ((1, 128),), -0.2, 0.2)), 0.005, 0.05)
    counts = plant(jax.random.randint(key_of[2], (ELEMS,), 1, SUBMAX + 1), jax.random.fold_in(key_of[2], 1), 1, SUBMAX).astype(jnp.int32)
    lame_first = jnp.clip(jnp.exp(math.log(2.0) - 1.3862944 * jax.random.uniform(key_of[3], (ELEMS,), jnp.float32) ** steps_of(key_of[3], (ELEMS,), ((0, 128),), -0.2, 0.2)), 0.5, 2.0)
    shear = jnp.clip(jnp.exp(math.log(2.0) - 1.3862944 * jax.random.uniform(key_of[4], (ELEMS,), jnp.float32) ** steps_of(key_of[4], (ELEMS,), ((0, 128),), -0.2, 0.2)), 0.5, 2.0)
    dest_owner_keys = jax.random.split(jax.random.fold_in(key_of[5], 1), ELEMS // E_DEV)
    dest_owner_turns = jax.random.permutation(jax.random.fold_in(key_of[5], 3), ELEMS // E_DEV)
    dest_owner = jax.vmap(lambda own, number: assign_block(jax.random.fold_in(key_of[5], 2), own, number, E_DEV, DEVICES, 1, CAP, 2))(dest_owner_keys, dest_owner_turns).reshape((ELEMS, 1))
    dest_slot = plant(jax.random.randint(key_of[6], (ELEMS,), 0, SLOTS_DEV), jax.random.fold_in(key_of[6], 1), 0, SLOTS_DEV - 1).astype(jnp.int32)
    return dict(grads=grads, weights=weights, counts=counts, lame_first=lame_first, shear=shear, dest_owner=dest_owner, dest_slot=dest_slot)


def stiffness(gflat, weff, lame_first, shear):
    count = gflat.shape[2]
    moment = jnp.einsum("qme,qne->mne", gflat * weff[:, None, :], gflat, precision=lax.Precision.HIGHEST)
    blocks = moment.reshape(NF, 3, NF, 3, count)
    across = jnp.einsum("akbke->abe", blocks)
    eye = jnp.eye(3, dtype=jnp.float32)
    result = lame_first * blocks + shear * (eye[None, :, None, :, None] * across[:, None, :, None, :] + jnp.transpose(blocks, (0, 3, 2, 1, 4)))
    return result.reshape(NDOF * NDOF, count)


def reference(grads, weights, counts, lame_first, shear, dest_owner, dest_slot):
    points = lax.broadcasted_iota(jnp.int32, weights.shape, 0)
    weff = jnp.where(points < counts[None, :] * GP, weights, jnp.float32(0.0))
    squares = jnp.sum(grads * grads, axis=(1, 2))
    total = jnp.sum((lame_first + 4.0 * shear) * jnp.sum(weff * squares, axis=0))
    scale = total / (NDOF * ELEMS)
    target = (dest_owner[:, 0] * SLOTS_DEV + dest_slot).astype(jnp.int32)
    gflat = grads.reshape(Q, NDOF, ELEMS)

    def add_block(index, accum):
        start = (index * E_DEV).astype(jnp.int32)
        gpart = lax.dynamic_slice_in_dim(gflat, start, E_DEV, 2)
        wpart = lax.dynamic_slice_in_dim(weff, start, E_DEV, 1)
        lpart = lax.dynamic_slice_in_dim(lame_first, start, E_DEV, 0)
        spart = lax.dynamic_slice_in_dim(shear, start, E_DEV, 0)
        tpart = lax.dynamic_slice_in_dim(target, start, E_DEV, 0)
        return accum.at[:, tpart].add(stiffness(gpart, wpart, lpart, spart))

    accum = lax.fori_loop(0, N_ROW * N_COL, add_block, jnp.zeros((NDOF * NDOF, SLOTS), jnp.float32))
    return (accum / scale).reshape(NDOF, NDOF, SLOTS)
```

```python
import functools

import jax
import jax.numpy as jnp
from jax import lax
from jax.experimental import pallas as pl
from jax.experimental.pallas import tpu as pltpu
from jax.sharding import PartitionSpec as P

NF = 20
NDOF = 60
Q = 64
NQB = 8
LANES = 128
CAP = 2
CHUNK = 512
ROWS = (8, 8, 8, 6)
PITCH = 20
OPITCH = 72
MESH = pl.DeviceIdType.MESH


def segments():
    table, row = {}, 1
    for a in range(NF):
        for i in range(3):
            for j in range(3):
                skip = 1 if i > j else 0
                table[a, i, j] = (row, skip)
                row += NF - a - skip
    return table, row


SEGMENTS, NWORDS = segments()
WORDS = 64 * CAP * 15
TRACE_LANE = NWORDS % LANES


def split_high_low(x, axis):
    high = x.astype(jnp.bfloat16)
    low = (x - high.astype(jnp.float32)).astype(jnp.bfloat16)
    return jnp.concatenate([high, low], axis=axis)


def exchange_kernel(
    ndev, ncol,
    grads_ref, weights_ref, counts_ref, lame_ref, shear_ref, owner_ref, slot_ref,
    placed_ref, total_ref,
    gbuf, gsem, weff, partial, kmat, permute, place, sendbuf, recvbuf, send_sem, recv_sem,
):
    row, col = lax.axis_index("row"), lax.axis_index("col")
    me = row * ncol + col

    barrier = pltpu.get_barrier_semaphore()

    def greet(k, carry):
        peer = lax.rem(me + k, ndev)
        pl.semaphore_signal(
            barrier, inc=1, device_id=(peer // ncol, lax.rem(peer, ncol)), device_id_type=MESH
        )
        return carry

    lax.fori_loop(1, ndev, greet, 0)

    load = pltpu.make_async_copy(grads_ref, gbuf, gsem)
    load.start()

    owner = owner_ref[...].astype(jnp.float32)
    wide = jnp.broadcast_to(owner, (LANES, LANES))
    rows_iota = lax.broadcasted_iota(jnp.int32, (LANES, LANES), 0)
    lane_iota = lax.broadcasted_iota(jnp.int32, (LANES, LANES), 1)
    same = jnp.where((wide.T == wide) & (rows_iota < lane_iota), 1.0, 0.0)
    rank = jnp.sum(same, axis=0, keepdims=True)
    here = rows_iota.astype(jnp.float32) == wide
    for r in range(CAP):
        onehot = jnp.where(here & (rank == float(r)), 1.0, 0.0).astype(jnp.bfloat16)
        permute[pl.ds(r * LANES, LANES), pl.ds(0, LANES)] = onehot
        permute[pl.ds(r * LANES, LANES), pl.ds(LANES, LANES)] = onehot

    counts = counts_ref[...]
    for qb in range(NQB):
        weff[pl.ds(8 * qb, 8), :] = jnp.where(
            counts > qb, weights_ref[pl.ds(8 * qb, 8), :], 0.0
        )
    lame, shear = lame_ref[...], shear_ref[...]
    kmat[pl.ds(0, 1), :] = slot_ref[...].astype(jnp.float32) + 1.0
    kmat[pl.ds(NWORDS, WORDS - NWORDS), :] = jnp.zeros((WORDS - NWORDS, LANES), jnp.float32)

    load.wait()

    def moments(a):
        gw = [
            [gbuf[3 * a + i, pl.ds(8 * qb, 8), :] * weff[pl.ds(8 * qb, 8), :] for qb in range(NQB)]
            for i in range(3)
        ]

        def one(b, carry):
            acc = [[None] * 3 for _ in range(3)]
            for qb in range(NQB):
                g = [gbuf[3 * b + j, pl.ds(8 * qb, 8), :] for j in range(3)]
                for i in range(3):
                    for j in range(3):
                        term = gw[i][qb] * g[j]
                        acc[i][j] = term if qb == 0 else acc[i][j] + term
            for i in range(3):
                for j in range(3):
                    partial[pl.ds((3 * i + j) * 8 * PITCH + b, 8, stride=PITCH), :] = acc[i][j]
            return carry

        lax.fori_loop(a, NF, one, 0)
        n = NF - a
        m = [[None] * 3 for _ in range(3)]
        for i in range(3):
            for j in range(3):
                base = (3 * i + j) * 8 * PITCH + a
                total = partial[pl.ds(base, n), :]
                for s in range(1, 8):
                    total = total + partial[pl.ds(base + s * PITCH, n), :]
                m[i][j] = total
        across = m[0][0] + m[1][1] + m[2][2]
        for i in range(3):
            for j in range(3):
                start, skip = SEGMENTS[a, i, j]
                if n == skip:
                    continue
                k = lame * m[i][j] + shear * (m[j][i] + across if i == j else m[j][i])
                kmat[pl.ds(start, n - skip), :] = k[skip:]
        return across[0:1]

    def pack(c, local_total):
        for j in range(ROWS[c] // CAP):
            words = kmat[pl.ds(c * CHUNK + j * LANES, LANES), :]
            out = lax.dot_general(
                permute[...], split_high_low(words, 1), (((1,), (1,)), ((), ())),
                preferred_element_type=jnp.float32,
            )
            for r in range(CAP):
                part = out[r * LANES:(r + 1) * LANES]
                if r == 0 and c == NWORDS // CHUNK and j == NWORDS % CHUNK // LANES:
                    part = jnp.where(lane_iota == TRACE_LANE, local_total, part)
                sendbuf[c, pl.ds(CAP * j + r, LANES, stride=8), :] = part
        own = pl.multiple_of(me * 8, 8)
        recvbuf[c, pl.ds(own, 8), :] = sendbuf[c, pl.ds(own, 8), :]

    def send(c):
        def one(k, carry):
            peer = lax.rem(me + lax.rem(k * 37, ndev), ndev)
            pltpu.make_async_remote_copy(
                src_ref=sendbuf.at[c, pl.ds(pl.multiple_of(peer * 8, 8), ROWS[c]), :],
                dst_ref=recvbuf.at[c, pl.ds(pl.multiple_of(me * 8, 8), ROWS[c]), :],
                send_sem=send_sem.at[c],
                recv_sem=recv_sem.at[c],
                device_id=(peer // ncol, lax.rem(peer, ncol)),
                device_id_type=MESH,
            ).start()
            return carry

        lax.fori_loop(1, ndev, one, 0)

    trace = jnp.zeros((1, LANES), jnp.float32)
    ready, a = 0, 0
    for c in range(len(ROWS)):
        need = min(c * CHUNK + CHUNK, NWORDS)
        while a < NF and SEGMENTS[a, 0, 0][0] < need:
            trace = trace + moments(a)
            a += 1
        pack(c, jnp.sum((lame + 4.0 * shear) * trace))
        if c == 0:
            pl.semaphore_wait(barrier, ndev - 1)
        send(c)

    def arrived(c):
        rows = (ndev - 1) * ROWS[c]
        pltpu.make_async_copy(
            recvbuf.at[c, pl.ds(0, rows), :], recvbuf.at[c, pl.ds(0, rows), :], recv_sem.at[c]
        ).wait()

    for c in range(len(ROWS)):
        arrived(c)
        for j in range(ROWS[c] // CAP):
            words = jnp.concatenate(
                [recvbuf[c, pl.ds(CAP * j + r, LANES, stride=8), :] for r in range(CAP)], axis=0
            )
            if c == 0 and j == 0:
                lanes = lax.broadcasted_iota(jnp.int32, (CAP * LANES, LANES), 1)
                hit = jnp.where(words[:, 0:1] - 1.0 == lanes.astype(jnp.float32), 1.0, 0.0)
                hit_t = jnp.concatenate([hit[0:LANES].T, hit[LANES:].T], axis=1)
                hit_t = hit_t.astype(jnp.bfloat16)
                place[...] = jnp.concatenate([hit_t, hit_t], axis=1)
            if c == NWORDS // CHUNK and j == NWORDS % CHUNK // LANES:
                total = jnp.sum(jnp.where(lane_iota == TRACE_LANE, words[0:LANES], 0.0))
                total_ref[...] = jnp.full(total_ref.shape, total, jnp.float32)
            out_t = jnp.dot(
                place[...], split_high_low(words, 0), preferred_element_type=jnp.float32
            )
            placed_ref[pl.ds(c * CHUNK + j * LANES, LANES), :] = out_t.T

    for c in range(len(ROWS)):
        rows = (ndev - 1) * ROWS[c]
        pltpu.make_async_copy(
            sendbuf.at[c, pl.ds(0, rows), :], sendbuf.at[c, pl.ds(0, rows), :], send_sem.at[c]
        ).wait()


def mirror_kernel(factor, placed_ref, total_ref, out_ref, planes, sems):
    inverse = factor / total_ref[0:1, :]
    copies = []
    for a in range(NF):
        for i in range(3):
            for j in range(3):
                start, skip = SEGMENTS[a, i, j]
                n, b = NF - a - skip, a + skip
                if n == 0:
                    continue
                values = placed_ref[pl.ds(start, n), :] * inverse
                planes[pl.ds((3 * a + i) * OPITCH + 3 * b + j, n, stride=3), :] = values
                planes[pl.ds((3 * b + j) * OPITCH + 3 * a + i, n, stride=3 * OPITCH), :] = values
        for i in range(3):
            m = 3 * a + i
            copy = pltpu.make_async_copy(
                planes.at[pl.ds(m * OPITCH, NDOF), :], out_ref.at[m], sems.at[m]
            )
            copy.start()
            copies.append(copy)
    for copy in copies:
        copy.wait()


def shards(nrow, ncol, grads, weights, counts, lame_first, shear, dest_owner, dest_slot):
    count = grads.shape[3]
    ndev = nrow * ncol
    vmem = pl.BlockSpec(memory_space=pltpu.VMEM)
    by_dof = jnp.transpose(grads, (1, 2, 0, 3)).reshape(NDOF, Q, count)
    placed, total = pl.pallas_call(
        functools.partial(exchange_kernel, ndev, ncol),
        out_shape=(
            jax.ShapeDtypeStruct((WORDS, LANES), jnp.float32),
            jax.ShapeDtypeStruct((8, LANES), jnp.float32),
        ),
        in_specs=[pl.BlockSpec(memory_space=pl.ANY)] + [vmem] * 6,
        out_specs=(vmem, vmem),
        scratch_shapes=[
            pltpu.VMEM((NDOF, Q, LANES), jnp.float32),
            pltpu.SemaphoreType.DMA,
            pltpu.VMEM((Q, LANES), jnp.float32),
            pltpu.VMEM((9 * 8 * PITCH + 24, LANES), jnp.float32),
            pltpu.VMEM((WORDS, LANES), jnp.float32),
            pltpu.VMEM((CAP * LANES, 2 * LANES), jnp.bfloat16),
            pltpu.VMEM((LANES, 2 * CAP * LANES), jnp.bfloat16),
            pltpu.VMEM((len(ROWS), LANES * 8 + 8, LANES), jnp.float32),
            pltpu.VMEM((len(ROWS), LANES * 8 + 8, LANES), jnp.float32),
            pltpu.SemaphoreType.DMA((len(ROWS),)),
            pltpu.SemaphoreType.DMA((len(ROWS),)),
        ],
        compiler_params=pltpu.CompilerParams(
            collective_id=0, has_side_effects=True, vmem_limit_bytes=24 << 20
        ),
    )(
        by_dof, weights, counts.reshape(1, count), lame_first.reshape(1, count),
        shear.reshape(1, count), dest_owner.reshape(1, count), dest_slot.reshape(1, count),
    )
    return pl.pallas_call(
        functools.partial(mirror_kernel, float(NDOF * count * ndev)),
        out_shape=jax.ShapeDtypeStruct((NDOF, NDOF, LANES), jnp.float32),
        in_specs=[vmem, vmem],
        out_specs=pl.BlockSpec(memory_space=pl.ANY),
        scratch_shapes=[
            pltpu.VMEM(((NDOF + 3) * OPITCH, LANES), jnp.float32),
            pltpu.SemaphoreType.DMA((NDOF,)),
        ],
        compiler_params=pltpu.CompilerParams(vmem_limit_bytes=16 << 20),
    )(placed, total)


def solution(mesh):
    axes = ("row", "col")
    return jax.shard_map(
        functools.partial(shards, mesh.shape["row"], mesh.shape["col"]),
        mesh=mesh,
        in_specs=(
            P(None, None, None, axes),
            P(None, axes),
            P(axes),
            P(axes),
            P(axes),
            P(axes, None),
            P(axes),
        ),
        out_specs=P(None, None, axes),
        check_vma=False,
    )
```

```python
import functools

import jax
import jax.numpy as jnp
from jax import lax
from jax.experimental import pallas as pl
from jax.experimental.pallas import tpu as pltpu
from jax.sharding import PartitionSpec as P

NF = 20
NDOF = 60
Q = 64
NQB = 8
LANES = 128
CAP = 2
CHUNK = 512
ROWS = (8, 8, 8, 6)
PITCH = 20
OPITCH = 72
MESH = pl.DeviceIdType.MESH


def segments():
    table, row = {}, 1
    for a in range(NF):
        for i in range(3):
            for j in range(3):
                skip = 1 if i > j else 0
                table[a, i, j] = (row, skip)
                row += NF - a - skip
    return table, row


SEGMENTS, NWORDS = segments()
WORDS = 64 * CAP * 15
TRACE_LANE = NWORDS % LANES


def split_high_low(x, axis):
    high = x.astype(jnp.bfloat16)
    low = (x - high.astype(jnp.float32)).astype(jnp.bfloat16)
    return jnp.concatenate([high, low], axis=axis)


def exchange_kernel(
    ndev, ncol,
    grads_hbm, weights_hbm, counts_hbm, lame_hbm, shear_hbm, owner_hbm, slot_hbm,
    placed_ref, total_ref,
    gbuf, weights_ref, counts_ref, lame_ref, shear_ref, owner_ref, slot_ref, load_sems, weff, partial, kmat, permute, place, sendbuf, recvbuf, send_sem, recv_sem,
):
    row, col = lax.axis_index("row"), lax.axis_index("col")
    me = row * ncol + col

    loads = [
        pltpu.make_async_copy(source, target, load_sems.at[k])
        for k, (source, target) in enumerate((
            (owner_hbm, owner_ref), (counts_hbm, counts_ref), (lame_hbm, lame_ref),
            (shear_hbm, shear_ref), (slot_hbm, slot_ref), (weights_hbm, weights_ref),
            (grads_hbm, gbuf),
        ))
    ]
    for load in loads:
        load.start()

    barrier = pltpu.get_barrier_semaphore()

    def greet(k, carry):
        peer = lax.rem(me + k, ndev)
        pl.semaphore_signal(
            barrier, inc=1, device_id=(peer // ncol, lax.rem(peer, ncol)), device_id_type=MESH
        )
        return carry

    lax.fori_loop(1, ndev, greet, 0)

    for load in loads[:-1]:
        load.wait()

    owner = owner_ref[...].astype(jnp.float32)
    wide = jnp.broadcast_to(owner, (LANES, LANES))
    rows_iota = lax.broadcasted_iota(jnp.int32, (LANES, LANES), 0)
    lane_iota = lax.broadcasted_iota(jnp.int32, (LANES, LANES), 1)
    same = jnp.where((wide.T == wide) & (rows_iota < lane_iota), 1.0, 0.0)
    rank = jnp.sum(same, axis=0, keepdims=True)
    here = rows_iota.astype(jnp.float32) == wide
    for r in range(CAP):
        onehot = jnp.where(here & (rank == float(r)), 1.0, 0.0).astype(jnp.bfloat16)
        permute[pl.ds(r * LANES, LANES), pl.ds(0, LANES)] = onehot
        permute[pl.ds(r * LANES, LANES), pl.ds(LANES, LANES)] = onehot

    counts = counts_ref[...]
    for qb in range(NQB):
        weff[pl.ds(8 * qb, 8), :] = jnp.where(
            counts > qb, weights_ref[pl.ds(8 * qb, 8), :], 0.0
        )
    lame, shear = lame_ref[...], shear_ref[...]
    kmat[pl.ds(0, 1), :] = slot_ref[...].astype(jnp.float32) + 1.0
    kmat[pl.ds(NWORDS, WORDS - NWORDS), :] = jnp.zeros((WORDS - NWORDS, LANES), jnp.float32)

    loads[-1].wait()

    def moments(a):
        gw = [
            [gbuf[3 * a + i, pl.ds(8 * qb, 8), :] * weff[pl.ds(8 * qb, 8), :] for qb in range(NQB)]
            for i in range(3)
        ]

        def one(b, carry):
            acc = [[None] * 3 for _ in range(3)]
            for qb in range(NQB):
                g = [gbuf[3 * b + j, pl.ds(8 * qb, 8), :] for j in range(3)]
                for i in range(3):
                    for j in range(3):
                        term = gw[i][qb] * g[j]
                        acc[i][j] = term if qb == 0 else acc[i][j] + term
            for i in range(3):
                for j in range(3):
                    partial[pl.ds((3 * i + j) * 8 * PITCH + b, 8, stride=PITCH), :] = acc[i][j]
            return carry

        lax.fori_loop(a, NF, one, 0)
        n = NF - a
        m = [[None] * 3 for _ in range(3)]
        for i in range(3):
            for j in range(3):
                base = (3 * i + j) * 8 * PITCH + a
                total = partial[pl.ds(base, n), :]
                for s in range(1, 8):
                    total = total + partial[pl.ds(base + s * PITCH, n), :]
                m[i][j] = total
        across = m[0][0] + m[1][1] + m[2][2]
        for i in range(3):
            for j in range(3):
                start, skip = SEGMENTS[a, i, j]
                if n == skip:
                    continue
                k = lame * m[i][j] + shear * (m[j][i] + across if i == j else m[j][i])
                kmat[pl.ds(start, n - skip), :] = k[skip:]
        return across[0:1]

    def pack(c, local_total):
        for j in range(ROWS[c] // CAP):
            words = kmat[pl.ds(c * CHUNK + j * LANES, LANES), :]
            out = lax.dot_general(
                permute[...], split_high_low(words, 1), (((1,), (1,)), ((), ())),
                preferred_element_type=jnp.float32,
            )
            for r in range(CAP):
                part = out[r * LANES:(r + 1) * LANES]
                if r == 0 and c == NWORDS // CHUNK and j == NWORDS % CHUNK // LANES:
                    part = jnp.where(lane_iota == TRACE_LANE, local_total, part)
                sendbuf[c, pl.ds(CAP * j + r, LANES, stride=8), :] = part
        own = pl.multiple_of(me * 8, 8)
        recvbuf[c, pl.ds(own, 8), :] = sendbuf[c, pl.ds(own, 8), :]

    def send(c):
        def one(k, carry):
            peer = lax.rem(me + lax.rem(k * 37, ndev), ndev)
            pltpu.make_async_remote_copy(
                src_ref=sendbuf.at[c, pl.ds(pl.multiple_of(peer * 8, 8), ROWS[c]), :],
                dst_ref=recvbuf.at[c, pl.ds(pl.multiple_of(me * 8, 8), ROWS[c]), :],
                send_sem=send_sem.at[c],
                recv_sem=recv_sem.at[c],
                device_id=(peer // ncol, lax.rem(peer, ncol)),
                device_id_type=MESH,
            ).start()
            return carry

        lax.fori_loop(1, ndev, one, 0)

    trace = jnp.zeros((1, LANES), jnp.float32)
    ready, a = 0, 0
    for c in range(len(ROWS)):
        need = min(c * CHUNK + CHUNK, NWORDS)
        while a < NF and SEGMENTS[a, 0, 0][0] < need:
            trace = trace + moments(a)
            a += 1
        pack(c, jnp.sum((lame + 4.0 * shear) * trace))
        if c == 0:
            pl.semaphore_wait(barrier, ndev - 1)
        send(c)

    def arrived(c):
        rows = (ndev - 1) * ROWS[c]
        pltpu.make_async_copy(
            recvbuf.at[c, pl.ds(0, rows), :], recvbuf.at[c, pl.ds(0, rows), :], recv_sem.at[c]
        ).wait()

    for c in range(len(ROWS)):
        arrived(c)
        for j in range(ROWS[c] // CAP):
            words = jnp.concatenate(
                [recvbuf[c, pl.ds(CAP * j + r, LANES, stride=8), :] for r in range(CAP)], axis=0
            )
            if c == 0 and j == 0:
                lanes = lax.broadcasted_iota(jnp.int32, (CAP * LANES, LANES), 1)
                hit = jnp.where(words[:, 0:1] - 1.0 == lanes.astype(jnp.float32), 1.0, 0.0)
                hit_t = jnp.concatenate([hit[0:LANES].T, hit[LANES:].T], axis=1)
                hit_t = hit_t.astype(jnp.bfloat16)
                place[...] = jnp.concatenate([hit_t, hit_t], axis=1)
            if c == NWORDS // CHUNK and j == NWORDS % CHUNK // LANES:
                total = jnp.sum(jnp.where(lane_iota == TRACE_LANE, words[0:LANES], 0.0))
                total_ref[...] = jnp.full(total_ref.shape, total, jnp.float32)
            out_t = jnp.dot(
                place[...], split_high_low(words, 0), preferred_element_type=jnp.float32
            )
            placed_ref[pl.ds(c * CHUNK + j * LANES, LANES), :] = out_t.T

    for c in range(len(ROWS)):
        rows = (ndev - 1) * ROWS[c]
        pltpu.make_async_copy(
            sendbuf.at[c, pl.ds(0, rows), :], sendbuf.at[c, pl.ds(0, rows), :], send_sem.at[c]
        ).wait()


def mirror_kernel(factor, placed_ref, total_ref, out_ref, planes, sems):
    inverse = factor / total_ref[0:1, :]
    copies = []
    for a in range(NF):
        for i in range(3):
            for j in range(3):
                start, skip = SEGMENTS[a, i, j]
                n, b = NF - a - skip, a + skip
                if n == 0:
                    continue
                values = placed_ref[pl.ds(start, n), :] * inverse
                planes[pl.ds((3 * a + i) * OPITCH + 3 * b + j, n, stride=3), :] = values
                planes[pl.ds((3 * b + j) * OPITCH + 3 * a + i, n, stride=3 * OPITCH), :] = values
        for i in range(3):
            m = 3 * a + i
            copy = pltpu.make_async_copy(
                planes.at[pl.ds(m * OPITCH, NDOF), :], out_ref.at[m], sems.at[m]
            )
            copy.start()
            copies.append(copy)
    for copy in copies:
        copy.wait()


def shards(nrow, ncol, grads, weights, counts, lame_first, shear, dest_owner, dest_slot):
    count = grads.shape[3]
    ndev = nrow * ncol
    vmem = pl.BlockSpec(memory_space=pltpu.VMEM)
    by_dof = jnp.transpose(grads, (1, 2, 0, 3)).reshape(NDOF, Q, count)
    placed, total = pl.pallas_call(
        functools.partial(exchange_kernel, ndev, ncol),
        out_shape=(
            jax.ShapeDtypeStruct((WORDS, LANES), jnp.float32),
            jax.ShapeDtypeStruct((8, LANES), jnp.float32),
        ),
        in_specs=[pl.BlockSpec(memory_space=pltpu.HBM)] * 7,
        out_specs=(vmem, vmem),
        scratch_shapes=[
            pltpu.VMEM((NDOF, Q, LANES), jnp.float32),
            pltpu.VMEM((Q, LANES), jnp.float32),
            pltpu.VMEM((1, LANES), jnp.int32),
            pltpu.VMEM((1, LANES), jnp.float32),
            pltpu.VMEM((1, LANES), jnp.float32),
            pltpu.VMEM((1, LANES), jnp.int32),
            pltpu.VMEM((1, LANES), jnp.int32),
            pltpu.SemaphoreType.DMA((7,)),
            pltpu.VMEM((Q, LANES), jnp.float32),
            pltpu.VMEM((9 * 8 * PITCH + 24, LANES), jnp.float32),
            pltpu.VMEM((WORDS, LANES), jnp.float32),
            pltpu.VMEM((CAP * LANES, 2 * LANES), jnp.bfloat16),
            pltpu.VMEM((LANES, 2 * CAP * LANES), jnp.bfloat16),
            pltpu.VMEM((len(ROWS), LANES * 8 + 8, LANES), jnp.float32),
            pltpu.VMEM((len(ROWS), LANES * 8 + 8, LANES), jnp.float32),
            pltpu.SemaphoreType.DMA((len(ROWS),)),
            pltpu.SemaphoreType.DMA((len(ROWS),)),
        ],
        compiler_params=pltpu.CompilerParams(
            collective_id=0, has_side_effects=True, vmem_limit_bytes=24 << 20
        ),
    )(
        by_dof, weights, counts.reshape(1, count), lame_first.reshape(1, count),
        shear.reshape(1, count), dest_owner.reshape(1, count), dest_slot.reshape(1, count),
    )
    return pl.pallas_call(
        functools.partial(mirror_kernel, float(NDOF * count * ndev)),
        out_shape=jax.ShapeDtypeStruct((NDOF, NDOF, LANES), jnp.float32),
        in_specs=[vmem, vmem],
        out_specs=pl.BlockSpec(memory_space=pl.ANY),
        scratch_shapes=[
            pltpu.VMEM(((NDOF + 3) * OPITCH, LANES), jnp.float32),
            pltpu.SemaphoreType.DMA((NDOF,)),
        ],
        compiler_params=pltpu.CompilerParams(vmem_limit_bytes=16 << 20),
    )(placed, total)


def solution(mesh):
    axes = ("row", "col")
    return jax.shard_map(
        functools.partial(shards, mesh.shape["row"], mesh.shape["col"]),
        mesh=mesh,
        in_specs=(
            P(None, None, None, axes),
            P(None, axes),
            P(axes),
            P(axes),
            P(axes),
            P(axes, None),
            P(axes),
        ),
        out_specs=P(None, None, axes),
        check_vma=False,
    )
```

```python
import functools

import jax
import jax.numpy as jnp
from jax import lax
from jax.experimental import pallas as pl
from jax.experimental.pallas import tpu as pltpu
from jax.sharding import PartitionSpec as P

NF = 20
NDOF = 60
Q = 64
NQB = 8
LANES = 128
CAP = 2
CHUNK = 512
ROWS = (8, 8, 8, 6)
PITCH = 20
OPITCH = 72
MESH = pl.DeviceIdType.MESH


def segments():
    table, row = {}, 1
    for a in range(NF):
        for i in range(3):
            for j in range(3):
                skip = 1 if i > j else 0
                table[a, i, j] = (row, skip)
                row += NF - a - skip
    return table, row


SEGMENTS, NWORDS = segments()
WORDS = 64 * CAP * 15
TRACE_LANE = NWORDS % LANES


def split_high_low(x, axis):
    high = x.astype(jnp.bfloat16)
    low = (x - high.astype(jnp.float32)).astype(jnp.bfloat16)
    return jnp.concatenate([high, low], axis=axis)


def exchange_kernel(
    ndev, ncol,
    grads_hbm, weights_hbm, counts_hbm, lame_hbm, shear_hbm, owner_hbm, slot_hbm,
    placed_ref, total_ref,
    gbuf, weights_ref, counts_ref, lame_ref, shear_ref, owner_ref, slot_ref, load_sems, weff, partial, kmat, permute, place, sendbuf, recvbuf, send_sem, recv_sem,
):
    row, col = lax.axis_index("row"), lax.axis_index("col")
    me = row * ncol + col

    loads = [
        pltpu.make_async_copy(source, target, load_sems.at[k])
        for k, (source, target) in enumerate((
            (owner_hbm, owner_ref), (counts_hbm, counts_ref), (lame_hbm, lame_ref),
            (shear_hbm, shear_ref), (slot_hbm, slot_ref), (weights_hbm, weights_ref),
            (grads_hbm, gbuf),
        ))
    ]
    for load in loads:
        load.start()

    barrier = pltpu.get_barrier_semaphore()

    def greet(k, carry):
        peer = lax.rem(me + k, ndev)
        pl.semaphore_signal(
            barrier, inc=1, device_id=(peer // ncol, lax.rem(peer, ncol)), device_id_type=MESH
        )
        return carry

    lax.fori_loop(1, ndev, greet, 0)

    for load in loads[:-1]:
        load.wait()

    owner = owner_ref[...].astype(jnp.float32)
    wide = jnp.broadcast_to(owner, (LANES, LANES))
    rows_iota = lax.broadcasted_iota(jnp.int32, (LANES, LANES), 0)
    lane_iota = lax.broadcasted_iota(jnp.int32, (LANES, LANES), 1)
    same = jnp.where((wide.T == wide) & (rows_iota < lane_iota), 1.0, 0.0)
    rank = jnp.sum(same, axis=0, keepdims=True)
    here = rows_iota.astype(jnp.float32) == wide
    for r in range(CAP):
        onehot = jnp.where(here & (rank == float(r)), 1.0, 0.0).astype(jnp.bfloat16)
        permute[pl.ds(r * LANES, LANES), pl.ds(0, LANES)] = onehot
        permute[pl.ds(r * LANES, LANES), pl.ds(LANES, LANES)] = onehot

    counts = counts_ref[...]
    for qb in range(NQB):
        weff[pl.ds(8 * qb, 8), :] = jnp.where(
            counts > qb, weights_ref[pl.ds(8 * qb, 8), :], 0.0
        )
    lame, shear = lame_ref[...], shear_ref[...]
    kmat[pl.ds(0, 1), :] = slot_ref[...].astype(jnp.float32) + 1.0
    kmat[pl.ds(NWORDS, WORDS - NWORDS), :] = jnp.zeros((WORDS - NWORDS, LANES), jnp.float32)

    loads[-1].wait()

    def moments(a):
        gw = [
            [gbuf[3 * a + i, pl.ds(8 * qb, 8), :] * weff[pl.ds(8 * qb, 8), :] for qb in range(NQB)]
            for i in range(3)
        ]

        def one(b, carry):
            acc = [[None] * 3 for _ in range(3)]
            for qb in range(NQB):
                g = [gbuf[3 * b + j, pl.ds(8 * qb, 8), :] for j in range(3)]
                for i in range(3):
                    for j in range(3):
                        term = gw[i][qb] * g[j]
                        acc[i][j] = term if qb == 0 else acc[i][j] + term
            for i in range(3):
                for j in range(3):
                    partial[pl.ds((3 * i + j) * 8 * PITCH + b, 8, stride=PITCH), :] = acc[i][j]
            return carry

        lax.fori_loop(a, NF, one, 0)
        n = NF - a
        m = [[None] * 3 for _ in range(3)]
        for i in range(3):
            for j in range(3):
                base = (3 * i + j) * 8 * PITCH + a
                total = partial[pl.ds(base, n), :]
                for s in range(1, 8):
                    total = total + partial[pl.ds(base + s * PITCH, n), :]
                m[i][j] = total
        across = m[0][0] + m[1][1] + m[2][2]
        for i in range(3):
            for j in range(3):
                start, skip = SEGMENTS[a, i, j]
                if n == skip:
                    continue
                k = lame * m[i][j] + shear * (m[j][i] + across if i == j else m[j][i])
                kmat[pl.ds(start, n - skip), :] = k[skip:]
        return across[0:1]

    def pack(c, local_total):
        for j in range(ROWS[c] // CAP):
            words = kmat[pl.ds(c * CHUNK + j * LANES, LANES), :]
            out = lax.dot_general(
                permute[...], split_high_low(words, 1), (((1,), (1,)), ((), ())),
                preferred_element_type=jnp.float32,
            )
            for r in range(CAP):
                part = out[r * LANES:(r + 1) * LANES]
                if r == 0 and c == NWORDS // CHUNK and j == NWORDS % CHUNK // LANES:
                    part = jnp.where(lane_iota == TRACE_LANE, local_total, part)
                sendbuf[c, pl.ds(CAP * j + r, LANES, stride=8), :] = part
        own = pl.multiple_of(me * 8, 8)
        recvbuf[c, pl.ds(own, 8), :] = sendbuf[c, pl.ds(own, 8), :]

    def send(c):
        def one(k, carry):
            peer = lax.rem(me + lax.rem(k * 37, ndev), ndev)
            pltpu.make_async_remote_copy(
                src_ref=sendbuf.at[c, pl.ds(pl.multiple_of(peer * 8, 8), ROWS[c]), :],
                dst_ref=recvbuf.at[c, pl.ds(pl.multiple_of(me * 8, 8), ROWS[c]), :],
                send_sem=send_sem.at[c],
                recv_sem=recv_sem.at[c],
                device_id=(peer // ncol, lax.rem(peer, ncol)),
                device_id_type=MESH,
            ).start()
            return carry

        lax.fori_loop(1, ndev, one, 0)

    trace = jnp.zeros((1, LANES), jnp.float32)
    ready, a = 0, 0
    for c in range(len(ROWS)):
        need = min(c * CHUNK + CHUNK, NWORDS)
        while a < NF and SEGMENTS[a, 0, 0][0] < need:
            trace = trace + moments(a)
            a += 1
        pack(c, jnp.sum((lame + 4.0 * shear) * trace))
        if c == 0:
            pl.semaphore_wait(barrier, ndev - 1)
        send(c)

    def arrived(c):
        rows = (ndev - 1) * ROWS[c]
        pltpu.make_async_copy(
            recvbuf.at[c, pl.ds(0, rows), :], recvbuf.at[c, pl.ds(0, rows), :], recv_sem.at[c]
        ).wait()

    for c in range(len(ROWS)):
        arrived(c)
        for j in range(ROWS[c] // CAP):
            words = jnp.concatenate(
                [recvbuf[c, pl.ds(CAP * j + r, LANES, stride=8), :] for r in range(CAP)], axis=0
            )
            if c == 0 and j == 0:
                lanes = lax.broadcasted_iota(jnp.int32, (CAP * LANES, LANES), 1)
                hit = jnp.where(words[:, 0:1] - 1.0 == lanes.astype(jnp.float32), 1.0, 0.0)
                hit_t = jnp.concatenate([hit[0:LANES].T, hit[LANES:].T], axis=1)
                hit_t = hit_t.astype(jnp.bfloat16)
                place[...] = jnp.concatenate([hit_t, hit_t], axis=1)
            if c == NWORDS // CHUNK and j == NWORDS % CHUNK // LANES:
                total = jnp.sum(jnp.where(lane_iota == TRACE_LANE, words[0:LANES], 0.0))
                total_ref[...] = jnp.full(total_ref.shape, total, jnp.float32)
            out_t = jnp.dot(
                place[...], split_high_low(words, 0), preferred_element_type=jnp.float32
            )
            placed_ref[pl.ds(c * CHUNK + j * LANES, LANES), :] = out_t.T

    for c in range(len(ROWS)):
        rows = (ndev - 1) * ROWS[c]
        pltpu.make_async_copy(
            sendbuf.at[c, pl.ds(0, rows), :], sendbuf.at[c, pl.ds(0, rows), :], send_sem.at[c]
        ).wait()


def mirror_kernel(factor, placed_ref, total_ref, out_ref, planes, sems):
    inverse = factor / total_ref[0:1, :]
    copies = []
    for a in range(NF):
        for i in range(3):
            for j in range(3):
                start, skip = SEGMENTS[a, i, j]
                n, b = NF - a - skip, a + skip
                if n == 0:
                    continue
                values = placed_ref[pl.ds(start, n), :] * inverse
                planes[pl.ds((3 * a + i) * OPITCH + 3 * b + j, n, stride=3), :] = values
                planes[pl.ds((3 * b + j) * OPITCH + 3 * a + i, n, stride=3 * OPITCH), :] = values
        for i in range(3):
            m = 3 * a + i
            copy = pltpu.make_async_copy(
                planes.at[pl.ds(m * OPITCH, NDOF), :], out_ref.at[m], sems.at[m]
            )
            copy.start()
            copies.append(copy)
    for copy in copies:
        copy.wait()


def shards(nrow, ncol, grads, weights, counts, lame_first, shear, dest_owner, dest_slot):
    count = grads.shape[3]
    ndev = nrow * ncol
    vmem = pl.BlockSpec(memory_space=pltpu.VMEM)
    by_dof = jnp.transpose(grads, (1, 2, 0, 3)).reshape(NDOF, Q, count)
    placed, total = pl.pallas_call(
        functools.partial(exchange_kernel, ndev, ncol),
        out_shape=(
            jax.ShapeDtypeStruct((WORDS, LANES), jnp.float32),
            jax.ShapeDtypeStruct((8, LANES), jnp.float32),
        ),
        in_specs=[pl.BlockSpec(memory_space=pltpu.HBM)] * 7,
        out_specs=(vmem, vmem),
        scratch_shapes=[
            pltpu.VMEM((NDOF, Q, LANES), jnp.float32),
            pltpu.VMEM((Q, LANES), jnp.float32),
            pltpu.VMEM((1, LANES), jnp.int32),
            pltpu.VMEM((1, LANES), jnp.float32),
            pltpu.VMEM((1, LANES), jnp.float32),
            pltpu.VMEM((1, LANES), jnp.int32),
            pltpu.VMEM((1, LANES), jnp.int32),
            pltpu.SemaphoreType.DMA((7,)),
            pltpu.VMEM((Q, LANES), jnp.float32),
            pltpu.VMEM((9 * 8 * PITCH + 24, LANES), jnp.float32),
            pltpu.VMEM((WORDS, LANES), jnp.float32),
            pltpu.VMEM((CAP * LANES, 2 * LANES), jnp.bfloat16),
            pltpu.VMEM((LANES, 2 * CAP * LANES), jnp.bfloat16),
            pltpu.VMEM((len(ROWS), LANES * 8 + 8, LANES), jnp.float32),
            pltpu.VMEM((len(ROWS), LANES * 8 + 8, LANES), jnp.float32),
            pltpu.SemaphoreType.DMA((len(ROWS),)),
            pltpu.SemaphoreType.DMA((len(ROWS),)),
        ],
        compiler_params=pltpu.CompilerParams(
            collective_id=0, has_side_effects=True, vmem_limit_bytes=24 << 20
        ),
    )(*(
        pltpu.with_memory_space_constraint(operand, pltpu.HBM)
        for operand in (
            by_dof, weights, counts.reshape(1, count), lame_first.reshape(1, count),
            shear.reshape(1, count), dest_owner.reshape(1, count), dest_slot.reshape(1, count),
        )
    ))
    return pl.pallas_call(
        functools.partial(mirror_kernel, float(NDOF * count * ndev)),
        out_shape=jax.ShapeDtypeStruct((NDOF, NDOF, LANES), jnp.float32),
        in_specs=[vmem, vmem],
        out_specs=pl.BlockSpec(memory_space=pl.ANY),
        scratch_shapes=[
            pltpu.VMEM(((NDOF + 3) * OPITCH, LANES), jnp.float32),
            pltpu.SemaphoreType.DMA((NDOF,)),
        ],
        compiler_params=pltpu.CompilerParams(vmem_limit_bytes=16 << 20),
    )(placed, total)


def solution(mesh):
    axes = ("row", "col")
    return jax.shard_map(
        functools.partial(shards, mesh.shape["row"], mesh.shape["col"]),
        mesh=mesh,
        in_specs=(
            P(None, None, None, axes),
            P(None, axes),
            P(axes),
            P(axes),
            P(axes),
            P(axes, None),
            P(axes),
        ),
        out_specs=P(None, None, axes),
        check_vma=False,
    )
```

```python
import functools

import jax
import jax.numpy as jnp
from jax import lax
from jax.experimental import pallas as pl
from jax.experimental.pallas import tpu as pltpu
from jax.sharding import PartitionSpec as P

NF = 20
NDOF = 60
Q = 64
NQB = 8
LANES = 128
CAP = 2
CHUNK = 512
ROWS = (8, 8, 8, 5)
PITCH = 20
OPITCH = 72
MESH = pl.DeviceIdType.MESH


def segments():
    table, row = {}, 2
    for a in range(NF):
        for i in range(3):
            for j in range(3):
                skip = 1 if i > j else 0
                table[a, i, j] = (row, skip)
                row += NF - a - skip
    return table, row


SEGMENTS, NWORDS = segments()
WORDS = 15 * LANES
HALF = LANES // 2


def split_high_low(x, axis):
    high = x.astype(jnp.bfloat16)
    low = (x - high.astype(jnp.float32)).astype(jnp.bfloat16)
    return jnp.concatenate([high, low], axis=axis)


def exchange_kernel(
    nrow, ncol,
    grads_hbm, weights_hbm, counts_hbm, lame_hbm, shear_hbm, owner_hbm, slot_hbm,
    planes_ref,
    gbuf, weights_ref, counts_ref, lame_ref, shear_ref, owner_ref, slot_ref, load_sems, weff, partial, kmat, placed, permute, place, sendbuf, recvbuf, send_sem, recv_sem,
):
    row, col = lax.axis_index("row"), lax.axis_index("col")
    me = row * ncol + col
    ndev = nrow * ncol

    loads = [
        pltpu.make_async_copy(source, target, load_sems.at[k])
        for k, (source, target) in enumerate((
            (owner_hbm, owner_ref), (counts_hbm, counts_ref), (lame_hbm, lame_ref),
            (shear_hbm, shear_ref), (slot_hbm, slot_ref), (weights_hbm, weights_ref),
            (grads_hbm, gbuf),
        ))
    ]
    for load in loads:
        load.start()

    barrier = pltpu.get_barrier_semaphore()

    rows_at = [lax.rem(row + k, nrow) for k in range(nrow)]
    cols_at = [lax.rem(col + k, ncol) for k in range(ncol)]
    for dr in range(nrow):
        for dc in range(ncol):
            if dr or dc:
                pl.semaphore_signal(
                    barrier, inc=1, device_id=(rows_at[dr], cols_at[dc]), device_id_type=MESH
                )

    for load in loads[:-1]:
        load.wait()

    owner = owner_ref[...].astype(jnp.float32)
    wide = jnp.broadcast_to(owner, (LANES, LANES))
    rows_iota = lax.broadcasted_iota(jnp.int32, (LANES, LANES), 0)
    lane_iota = lax.broadcasted_iota(jnp.int32, (LANES, LANES), 1)
    same = jnp.where((wide.T == wide) & (rows_iota < lane_iota), 1.0, 0.0)
    rank = jnp.sum(same, axis=0, keepdims=True)
    here = rows_iota.astype(jnp.float32) == wide
    for r in range(CAP):
        onehot = jnp.where(here & (rank == float(r)), 1.0, 0.0).astype(jnp.bfloat16)
        permute[pl.ds(r * LANES, LANES), pl.ds(0, LANES)] = onehot
        permute[pl.ds(r * LANES, LANES), pl.ds(LANES, LANES)] = onehot

    counts = counts_ref[...]
    for qb in range(NQB):
        weff[pl.ds(8 * qb, 8), :] = jnp.where(
            counts > qb, weights_ref[pl.ds(8 * qb, 8), :], 0.0
        )
    lame, shear = lame_ref[...], shear_ref[...]
    kmat[pl.ds(0, 1), :] = slot_ref[...].astype(jnp.float32) + 1.0
    kmat[pl.ds(NWORDS, WORDS - NWORDS), :] = jnp.zeros((WORDS - NWORDS, LANES), jnp.float32)

    loads[-1].wait()

    def moments(a):
        gw = [
            [gbuf[3 * a + i, pl.ds(8 * qb, 8), :] * weff[pl.ds(8 * qb, 8), :] for qb in range(NQB)]
            for i in range(3)
        ]

        def one(b, carry):
            acc = [[None] * 3 for _ in range(3)]
            for qb in range(NQB):
                g = [gbuf[3 * b + j, pl.ds(8 * qb, 8), :] for j in range(3)]
                for i in range(3):
                    for j in range(3):
                        term = gw[i][qb] * g[j]
                        acc[i][j] = term if qb == 0 else acc[i][j] + term
            for i in range(3):
                for j in range(3):
                    partial[pl.ds((3 * i + j) * 8 * PITCH + b, 8, stride=PITCH), :] = acc[i][j]
            return carry

        lax.fori_loop(a, NF, one, 0)
        n = NF - a
        m = [[None] * 3 for _ in range(3)]
        for i in range(3):
            for j in range(3):
                base = (3 * i + j) * 8 * PITCH + a
                total = partial[pl.ds(base, n), :]
                for s in range(1, 8):
                    total = total + partial[pl.ds(base + s * PITCH, n), :]
                m[i][j] = total
        across = m[0][0] + m[1][1] + m[2][2]
        for i in range(3):
            for j in range(3):
                start, skip = SEGMENTS[a, i, j]
                if n == skip:
                    continue
                k = lame * m[i][j] + shear * (m[j][i] + across if i == j else m[j][i])
                kmat[pl.ds(start, n - skip), :] = k[skip:]

    def pack(c):
        for j in range((ROWS[c] + 1) // CAP):
            words = kmat[pl.ds(c * CHUNK + j * LANES, LANES), :]
            out = lax.dot_general(
                permute[...], split_high_low(words, 1), (((1,), (1,)), ((), ())),
                preferred_element_type=jnp.float32,
            )
            parts = [out[r * LANES:(r + 1) * LANES] for r in range(CAP)]
            if c == 0 and j == 0:
                parts[0] = jnp.where(lane_iota == 1, local_trace, parts[0])
            if CAP * (j + 1) > ROWS[c]:
                parts = [parts[0] + pltpu.roll(parts[1], HALF, 1)]
            for r, part in enumerate(parts):
                sendbuf[c, pl.ds(CAP * j + r, LANES, stride=8), :] = part
        own = pl.multiple_of(me * 8, 8)
        recvbuf[c, pl.ds(own, 8), :] = sendbuf[c, pl.ds(own, 8), :]

    def send(c):
        def to(peer_row, dc):
            peer = peer_row * ncol + cols_at[dc]
            pltpu.make_async_remote_copy(
                src_ref=sendbuf.at[c, pl.ds(pl.multiple_of(peer * 8, 8), ROWS[c]), :],
                dst_ref=recvbuf.at[c, pl.ds(pl.multiple_of(me * 8, 8), ROWS[c]), :],
                send_sem=send_sem.at[c],
                recv_sem=recv_sem.at[c],
                device_id=(peer_row, cols_at[dc]),
                device_id_type=MESH,
            ).start()

        def to_row(dr, carry):
            peer_row = lax.rem(row + dr, nrow)
            for dc in range(ncol):
                to(peer_row, dc)
            return carry

        lax.fori_loop(1, nrow, to_row, 0)
        for dc in range(1, ncol):
            to(row, dc)

    squares = [jnp.zeros((8, LANES), jnp.float32)] * NQB
    for m in range(NDOF):
        for qb in range(NQB):
            g = gbuf[m, pl.ds(8 * qb, 8), :]
            squares[qb] = squares[qb] + g * g
    weighted = sum(weff[pl.ds(8 * qb, 8), :] * squares[qb] for qb in range(NQB))
    local_trace = jnp.sum((lame + 4.0 * shear) * weighted)

    a = 0
    for c in range(len(ROWS)):
        need = min(c * CHUNK + CHUNK, NWORDS)
        while a < NF and SEGMENTS[a, 0, 0][0] < need:
            moments(a)
            a += 1
        pack(c)
        if c == 0:
            pl.semaphore_wait(barrier, ndev - 1)
        send(c)

    def arrived(c):
        rows = (ndev - 1) * ROWS[c]
        pltpu.make_async_copy(
            recvbuf.at[c, pl.ds(0, rows), :], recvbuf.at[c, pl.ds(0, rows), :], recv_sem.at[c]
        ).wait()

    inverse = None
    pending = [key for key in SEGMENTS if NF - key[0] > SEGMENTS[key][1]]
    for c in range(len(ROWS)):
        arrived(c)
        for j in range((ROWS[c] + 1) // CAP):
            if CAP * (j + 1) > ROWS[c]:
                shared = recvbuf[c, pl.ds(CAP * j, LANES, stride=8), :]
                parts = [shared, pltpu.roll(shared, HALF, 1)]
            else:
                parts = [recvbuf[c, pl.ds(CAP * j + r, LANES, stride=8), :] for r in range(CAP)]
            words = jnp.concatenate(parts, axis=0)
            if c == 0 and j == 0:
                lanes = lax.broadcasted_iota(jnp.int32, (CAP * LANES, LANES), 1)
                hit = jnp.where(words[:, 0:1] - 1.0 == lanes.astype(jnp.float32), 1.0, 0.0)
                hit_t = jnp.concatenate([hit[0:LANES].T, hit[LANES:].T], axis=1)
                hit_t = hit_t.astype(jnp.bfloat16)
                place[...] = jnp.concatenate([hit_t, hit_t], axis=1)
                total = jnp.sum(parts[0][:, 1:2], axis=0, keepdims=True)
                inverse = jnp.broadcast_to(float(NDOF * LANES * ndev) / total, (8, LANES))
            out_t = jnp.dot(
                place[...], split_high_low(words, 0), preferred_element_type=jnp.float32
            )
            placed[pl.ds(c * CHUNK + j * LANES, LANES), :] = out_t.T
        while pending:
            a, i, j = pending[0]
            start, skip = SEGMENTS[a, i, j]
            n, b = NF - a - skip, a + skip
            if c < len(ROWS) - 1 and start + n > (c + 1) * CHUNK:
                break
            pending.pop(0)
            values = placed[pl.ds(start, n), :] * inverse[0:1]
            planes_ref[pl.ds((3 * a + i) * OPITCH + 3 * b + j, n, stride=3), :] = values
            planes_ref[pl.ds((3 * b + j) * OPITCH + 3 * a + i, n, stride=3 * OPITCH), :] = values

    for c in range(len(ROWS)):
        rows = (ndev - 1) * ROWS[c]
        pltpu.make_async_copy(
            sendbuf.at[c, pl.ds(0, rows), :], sendbuf.at[c, pl.ds(0, rows), :], send_sem.at[c]
        ).wait()


def copy_out_kernel(planes_ref, out_ref, sems):
    copies = [
        pltpu.make_async_copy(
            planes_ref.at[pl.ds(m * OPITCH, NDOF), :], out_ref.at[m], sems.at[m]
        )
        for m in range(NDOF)
    ]
    for copy in copies:
        copy.start()
    for copy in copies:
        copy.wait()


def shards(nrow, ncol, grads, weights, counts, lame_first, shear, dest_owner, dest_slot):
    count = grads.shape[3]
    vmem = pl.BlockSpec(memory_space=pltpu.VMEM)
    by_dof = jnp.transpose(grads, (1, 2, 0, 3)).reshape(NDOF, Q, count)
    planes = pl.pallas_call(
        functools.partial(exchange_kernel, nrow, ncol),
        out_shape=jax.ShapeDtypeStruct(((NDOF + 4) * OPITCH, LANES), jnp.float32),
        in_specs=[pl.BlockSpec(memory_space=pltpu.HBM)] * 7,
        out_specs=vmem,
        scratch_shapes=[
            pltpu.VMEM((NDOF, Q, LANES), jnp.float32),
            pltpu.VMEM((Q, LANES), jnp.float32),
            pltpu.VMEM((1, LANES), jnp.int32),
            pltpu.VMEM((1, LANES), jnp.float32),
            pltpu.VMEM((1, LANES), jnp.float32),
            pltpu.VMEM((1, LANES), jnp.int32),
            pltpu.VMEM((1, LANES), jnp.int32),
            pltpu.SemaphoreType.DMA((7,)),
            pltpu.VMEM((Q, LANES), jnp.float32),
            pltpu.VMEM((9 * 8 * PITCH + 24, LANES), jnp.float32),
            pltpu.VMEM((WORDS, LANES), jnp.float32),
            pltpu.VMEM((WORDS, LANES), jnp.float32),
            pltpu.VMEM((CAP * LANES, 2 * LANES), jnp.bfloat16),
            pltpu.VMEM((LANES, 2 * CAP * LANES), jnp.bfloat16),
            pltpu.VMEM((len(ROWS), LANES * 8 + 8, LANES), jnp.float32),
            pltpu.VMEM((len(ROWS), LANES * 8 + 8, LANES), jnp.float32),
            pltpu.SemaphoreType.DMA((len(ROWS),)),
            pltpu.SemaphoreType.DMA((len(ROWS),)),
        ],
        compiler_params=pltpu.CompilerParams(
            collective_id=0, has_side_effects=True, vmem_limit_bytes=24 << 20
        ),
    )(*(
        pltpu.with_memory_space_constraint(operand, pltpu.HBM)
        for operand in (
            by_dof, weights, counts.reshape(1, count), lame_first.reshape(1, count),
            shear.reshape(1, count), dest_owner.reshape(1, count), dest_slot.reshape(1, count),
        )
    ))
    return pl.pallas_call(
        copy_out_kernel,
        out_shape=jax.ShapeDtypeStruct((NDOF, NDOF, LANES), jnp.float32),
        in_specs=[vmem],
        out_specs=pl.BlockSpec(memory_space=pl.ANY),
        scratch_shapes=[pltpu.SemaphoreType.DMA((NDOF,))],
        compiler_params=pltpu.CompilerParams(vmem_limit_bytes=16 << 20),
    )(planes)


def solution(mesh):
    axes = ("row", "col")
    return jax.shard_map(
        functools.partial(shards, mesh.shape["row"], mesh.shape["col"]),
        mesh=mesh,
        in_specs=(
            P(None, None, None, axes),
            P(None, axes),
            P(axes),
            P(axes),
            P(axes),
            P(axes, None),
            P(axes),
        ),
        out_specs=P(None, None, axes),
        check_vma=False,
    )
```

```python
import functools

import jax
import jax.numpy as jnp
from jax import lax
from jax.experimental import pallas as pl
from jax.experimental.pallas import tpu as pltpu
from jax.sharding import PartitionSpec as P

NF = 20
NDOF = 60
Q = 64
NQB = 8
LANES = 128
CAP = 2
CHUNK = 512
ROWS = (8, 8, 8, 5)
PITCH = 20
MESH = pl.DeviceIdType.MESH
COL_ORDER = (4, 5, 2, 3, 6, 7, 0, 1)


def segments():
    table, row = {}, 2
    for a in range(NF):
        for i in range(3):
            for j in range(3):
                skip = 1 if i > j else 0
                table[a, i, j] = (row, skip)
                row += NF - a - skip
    return table, row


SEGMENTS, NWORDS = segments()
WORDS = 15 * LANES
HALF = LANES // 2


def split_high_low(x, axis):
    high = x.astype(jnp.bfloat16)
    low = (x - high.astype(jnp.float32)).astype(jnp.bfloat16)
    return jnp.concatenate([high, low], axis=axis)


def exchange_kernel(
    nrow, ncol,
    grads_hbm, weights_hbm, counts_hbm, lame_hbm, shear_hbm, owner_hbm, slot_hbm,
    planes_ref,
    gbuf, weights_ref, counts_ref, lame_ref, shear_ref, owner_ref, slot_ref, load_sems, weff, partial, kmat, placed, permute, place, sendbuf, recvbuf, send_sem, recv_sem,
):
    row, col = lax.axis_index("row"), lax.axis_index("col")
    me = row * ncol + col
    ndev = nrow * ncol

    loads = [
        pltpu.make_async_copy(source, target, load_sems.at[k])
        for k, (source, target) in enumerate((
            (owner_hbm, owner_ref), (counts_hbm, counts_ref), (lame_hbm, lame_ref),
            (shear_hbm, shear_ref), (slot_hbm, slot_ref), (weights_hbm, weights_ref),
            (grads_hbm, gbuf),
        ))
    ]
    for load in loads:
        load.start()

    barrier = pltpu.get_barrier_semaphore()

    rows_at = [lax.rem(row + k, nrow) for k in range(nrow)]
    cols_at = [lax.rem(col + k, ncol) for k in range(ncol)]
    hops = (0, 1, 2, 1)
    order = sorted(
        ((dr, dc) for dr in range(nrow) for dc in range(ncol) if dr or dc),
        key=lambda o: -(hops[o[0] // 4] + hops[o[0] % 4] + hops[o[1] // 2]),
    )
    for dr, dc in order:
        pl.semaphore_signal(
            barrier, inc=1, device_id=(rows_at[dr], cols_at[dc]), device_id_type=MESH
        )

    for load in loads[:-1]:
        load.wait()

    owner = owner_ref[...].astype(jnp.float32)
    wide = jnp.broadcast_to(owner, (LANES, LANES))
    rows_iota = lax.broadcasted_iota(jnp.int32, (LANES, LANES), 0)
    lane_iota = lax.broadcasted_iota(jnp.int32, (LANES, LANES), 1)
    same = jnp.where((wide.T == wide) & (rows_iota < lane_iota), 1.0, 0.0)
    rank = jnp.sum(same, axis=0, keepdims=True)
    here = rows_iota.astype(jnp.float32) == wide
    for r in range(CAP):
        onehot = jnp.where(here & (rank == float(r)), 1.0, 0.0).astype(jnp.bfloat16)
        permute[pl.ds(r * LANES, LANES), pl.ds(0, LANES)] = onehot
        permute[pl.ds(r * LANES, LANES), pl.ds(LANES, LANES)] = onehot

    counts = counts_ref[...]
    for qb in range(NQB):
        weff[pl.ds(8 * qb, 8), :] = jnp.where(
            counts > qb, weights_ref[pl.ds(8 * qb, 8), :], 0.0
        )
    lame, shear = lame_ref[...], shear_ref[...]
    kmat[pl.ds(0, 8), :] = jnp.zeros((8, LANES), jnp.float32)
    kmat[pl.ds(0, 1), :] = slot_ref[...].astype(jnp.float32) + 1.0
    kmat[pl.ds(NWORDS, WORDS - NWORDS), :] = jnp.zeros((WORDS - NWORDS, LANES), jnp.float32)

    loads[-1].wait()

    def moments(a):
        gw = [
            [gbuf[3 * a + i, pl.ds(8 * qb, 8), :] * weff[pl.ds(8 * qb, 8), :] for qb in range(NQB)]
            for i in range(3)
        ]

        def one(b, carry):
            acc = [[None] * 3 for _ in range(3)]
            for qb in range(NQB):
                g = [gbuf[3 * b + j, pl.ds(8 * qb, 8), :] for j in range(3)]
                for i in range(3):
                    for j in range(3):
                        term = gw[i][qb] * g[j]
                        acc[i][j] = term if qb == 0 else acc[i][j] + term
            for i in range(3):
                for j in range(3):
                    partial[pl.ds((3 * i + j) * 8 * PITCH + b, 8, stride=PITCH), :] = acc[i][j]
            return carry

        lax.fori_loop(a, NF, one, 0)
        n = NF - a
        m = [[None] * 3 for _ in range(3)]
        for i in range(3):
            for j in range(3):
                base = (3 * i + j) * 8 * PITCH + a
                total = partial[pl.ds(base, n), :]
                for s in range(1, 8):
                    total = total + partial[pl.ds(base + s * PITCH, n), :]
                m[i][j] = total
        across = m[0][0] + m[1][1] + m[2][2]
        for i in range(3):
            for j in range(3):
                start, skip = SEGMENTS[a, i, j]
                if n == skip:
                    continue
                k = lame * m[i][j] + shear * (m[j][i] + across if i == j else m[j][i])
                kmat[pl.ds(start, n - skip), :] = k[skip:]

    def pack(c):
        for j in range((ROWS[c] + 1) // CAP):
            words = kmat[pl.ds(c * CHUNK + j * LANES, LANES), :]
            out = lax.dot_general(
                permute[...], split_high_low(words, 1), (((1,), (1,)), ((), ())),
                preferred_element_type=jnp.float32,
            )
            parts = [out[r * LANES:(r + 1) * LANES] for r in range(CAP)]
            if c == 0 and j == 0:
                parts[0] = jnp.where(lane_iota == 1, local_trace, parts[0])
            if CAP * (j + 1) > ROWS[c]:
                parts = [parts[0] + pltpu.roll(parts[1], HALF, 1)]
            for r, part in enumerate(parts):
                sendbuf[c, pl.ds(CAP * j + r, LANES, stride=8), :] = part
        own = pl.multiple_of(me * 8, 8)
        recvbuf[c, pl.ds(own, 8), :] = sendbuf[c, pl.ds(own, 8), :]

    def send(c):
        def to(peer_row, dc):
            peer = peer_row * ncol + cols_at[dc]
            pltpu.make_async_remote_copy(
                src_ref=sendbuf.at[c, pl.ds(pl.multiple_of(peer * 8, 8), ROWS[c]), :],
                dst_ref=recvbuf.at[c, pl.ds(pl.multiple_of(me * 8, 8), ROWS[c]), :],
                send_sem=send_sem.at[c],
                recv_sem=recv_sem.at[c],
                device_id=(peer_row, cols_at[dc]),
                device_id_type=MESH,
            ).start()

        def to_row(k, carry):
            peer_row = lax.rem(row + k, nrow)
            for dc in COL_ORDER:
                to(peer_row, dc)
            return carry

        lax.fori_loop(1, nrow, to_row, 0)
        for dc in range(1, ncol):
            to(row, dc)

    squares = [jnp.zeros((8, LANES), jnp.float32)] * NQB
    for m in range(NDOF):
        for qb in range(NQB):
            g = gbuf[m, pl.ds(8 * qb, 8), :]
            squares[qb] = squares[qb] + g * g
    weighted = sum(weff[pl.ds(8 * qb, 8), :] * squares[qb] for qb in range(NQB))
    local_trace = jnp.sum((lame + 4.0 * shear) * weighted)

    a = 0
    for c in range(len(ROWS)):
        need = min(c * CHUNK + CHUNK, NWORDS)
        while a < NF and SEGMENTS[a, 0, 0][0] < need:
            moments(a)
            a += 1
        pack(c)
        if c == 0:
            pl.semaphore_wait(barrier, ndev - 1)
        send(c)

    def arrived(c):
        rows = (ndev - 1) * ROWS[c]
        pltpu.make_async_copy(
            recvbuf.at[c, pl.ds(0, rows), :], recvbuf.at[c, pl.ds(0, rows), :], recv_sem.at[c]
        ).wait()

    inverse = None
    pending = [key for key in SEGMENTS if NF - key[0] > SEGMENTS[key][1]]
    for c in range(len(ROWS)):
        arrived(c)
        for j in range((ROWS[c] + 1) // CAP):
            if CAP * (j + 1) > ROWS[c]:
                shared = recvbuf[c, pl.ds(CAP * j, LANES, stride=8), :]
                parts = [shared, pltpu.roll(shared, HALF, 1)]
            else:
                parts = [recvbuf[c, pl.ds(CAP * j + r, LANES, stride=8), :] for r in range(CAP)]
            words = jnp.concatenate(parts, axis=0)
            if c == 0 and j == 0:
                lanes = lax.broadcasted_iota(jnp.int32, (CAP * LANES, LANES), 1)
                hit = jnp.where(words[:, 0:1] - 1.0 == lanes.astype(jnp.float32), 1.0, 0.0)
                hit_t = jnp.concatenate([hit[0:LANES].T, hit[LANES:].T], axis=1)
                hit_t = hit_t.astype(jnp.bfloat16)
                place[...] = jnp.concatenate([hit_t, hit_t], axis=1)
                total = jnp.sum(parts[0][:, 1:2], axis=0, keepdims=True)
                inverse = jnp.broadcast_to(float(NDOF * LANES * ndev) / total, (8, LANES))
            out_t = jnp.dot(
                place[...], split_high_low(words, 0), preferred_element_type=jnp.float32
            )
            placed[pl.ds(c * CHUNK + j * LANES, LANES), :] = out_t.T
        while pending:
            a, i, j = pending[0]
            start, skip = SEGMENTS[a, i, j]
            n, b = NF - a - skip, a + skip
            if c < len(ROWS) - 1 and start + n > (c + 1) * CHUNK:
                break
            pending.pop(0)
            values = placed[pl.ds(start, n), :] * inverse[0:1]
            planes_ref[3 * a + i, pl.ds(3 * b + j, n, stride=3), :] = values
            for t in range(n):
                planes_ref[3 * (b + t) + j, pl.ds(3 * a + i, 1), :] = values[t:t + 1]

    for c in range(len(ROWS)):
        rows = (ndev - 1) * ROWS[c]
        pltpu.make_async_copy(
            sendbuf.at[c, pl.ds(0, rows), :], sendbuf.at[c, pl.ds(0, rows), :], send_sem.at[c]
        ).wait()


def shards(nrow, ncol, grads, weights, counts, lame_first, shear, dest_owner, dest_slot):
    count = grads.shape[3]
    vmem = pl.BlockSpec(memory_space=pltpu.VMEM)
    by_dof = jnp.transpose(grads, (1, 2, 0, 3)).reshape(NDOF, Q, count)
    return pl.pallas_call(
        functools.partial(exchange_kernel, nrow, ncol),
        out_shape=jax.ShapeDtypeStruct((NDOF, NDOF, LANES), jnp.float32),
        in_specs=[pl.BlockSpec(memory_space=pltpu.HBM)] * 7,
        out_specs=vmem,
        scratch_shapes=[
            pltpu.VMEM((NDOF, Q, LANES), jnp.float32),
            pltpu.VMEM((Q, LANES), jnp.float32),
            pltpu.VMEM((1, LANES), jnp.int32),
            pltpu.VMEM((1, LANES), jnp.float32),
            pltpu.VMEM((1, LANES), jnp.float32),
            pltpu.VMEM((1, LANES), jnp.int32),
            pltpu.VMEM((1, LANES), jnp.int32),
            pltpu.SemaphoreType.DMA((7,)),
            pltpu.VMEM((Q, LANES), jnp.float32),
            pltpu.VMEM((9 * 8 * PITCH + 24, LANES), jnp.float32),
            pltpu.VMEM((WORDS, LANES), jnp.float32),
            pltpu.VMEM((WORDS, LANES), jnp.float32),
            pltpu.VMEM((CAP * LANES, 2 * LANES), jnp.bfloat16),
            pltpu.VMEM((LANES, 2 * CAP * LANES), jnp.bfloat16),
            pltpu.VMEM((len(ROWS), LANES * 8 + 8, LANES), jnp.float32),
            pltpu.VMEM((len(ROWS), LANES * 8 + 8, LANES), jnp.float32),
            pltpu.SemaphoreType.DMA((len(ROWS),)),
            pltpu.SemaphoreType.DMA((len(ROWS),)),
        ],
        compiler_params=pltpu.CompilerParams(
            collective_id=0, has_side_effects=True, vmem_limit_bytes=24 << 20
        ),
    )(*(
        pltpu.with_memory_space_constraint(operand, pltpu.HBM)
        for operand in (
            by_dof, weights, counts.reshape(1, count), lame_first.reshape(1, count),
            shear.reshape(1, count), dest_owner.reshape(1, count), dest_slot.reshape(1, count),
        )
    ))


def solution(mesh):
    axes = ("row", "col")
    return jax.shard_map(
        functools.partial(shards, mesh.shape["row"], mesh.shape["col"]),
        mesh=mesh,
        in_specs=(
            P(None, None, None, axes),
            P(None, axes),
            P(axes),
            P(axes),
            P(axes),
            P(axes, None),
            P(axes),
        ),
        out_specs=P(None, None, axes),
        check_vma=False,
    )
```

```python
import functools

import jax
import jax.numpy as jnp
from jax import lax
from jax.experimental import pallas as pl
from jax.experimental.pallas import tpu as pltpu
from jax.sharding import PartitionSpec as P

NF = 20
NDOF = 60
Q = 64
NQB = 8
LANES = 128
CAP = 2
ROWS = (6, 6, 6, 6, 5)
STARTS = tuple(LANES * (sum(ROWS[:c]) // CAP) for c in range(len(ROWS)))
PITCH = 20
MESH = pl.DeviceIdType.MESH
COL_ORDER = (4, 5, 2, 3, 6, 7, 0, 1)


def segments():
    table, row = {}, 2
    for a in range(NF):
        for i in range(3):
            for j in range(3):
                skip = 1 if i > j else 0
                table[a, i, j] = (row, skip)
                row += NF - a - skip
    return table, row


SEGMENTS, NWORDS = segments()
WORDS = 15 * LANES
HALF = LANES // 2


def split_high_low(x, axis):
    high = x.astype(jnp.bfloat16)
    low = (x - high.astype(jnp.float32)).astype(jnp.bfloat16)
    return jnp.concatenate([high, low], axis=axis)


def exchange_kernel(
    nrow, ncol,
    grads_hbm, weights_hbm, counts_hbm, lame_hbm, shear_hbm, owner_hbm, slot_hbm,
    planes_ref,
    gbuf, weights_ref, counts_ref, lame_ref, shear_ref, owner_ref, slot_ref, load_sems, weff, partial, kmat, placed, permute, place, sendbuf, recvbuf, send_sem, recv_sem,
):
    row, col = lax.axis_index("row"), lax.axis_index("col")
    me = row * ncol + col
    ndev = nrow * ncol

    loads = [
        pltpu.make_async_copy(source, target, load_sems.at[k])
        for k, (source, target) in enumerate((
            (owner_hbm, owner_ref), (counts_hbm, counts_ref), (lame_hbm, lame_ref),
            (shear_hbm, shear_ref), (slot_hbm, slot_ref), (weights_hbm, weights_ref),
            (grads_hbm, gbuf),
        ))
    ]
    for load in loads:
        load.start()

    barrier = pltpu.get_barrier_semaphore()

    rows_at = [lax.rem(row + k, nrow) for k in range(nrow)]
    cols_at = [lax.rem(col + k, ncol) for k in range(ncol)]
    hops = (0, 1, 2, 1)
    order = sorted(
        ((dr, dc) for dr in range(nrow) for dc in range(ncol) if dr or dc),
        key=lambda o: -(hops[o[0] // 4] + hops[o[0] % 4] + hops[o[1] // 2]),
    )
    for dr, dc in order:
        pl.semaphore_signal(
            barrier, inc=1, device_id=(rows_at[dr], cols_at[dc]), device_id_type=MESH
        )

    for load in loads[:-1]:
        load.wait()

    owner = owner_ref[...].astype(jnp.float32)
    wide = jnp.broadcast_to(owner, (LANES, LANES))
    rows_iota = lax.broadcasted_iota(jnp.int32, (LANES, LANES), 0)
    lane_iota = lax.broadcasted_iota(jnp.int32, (LANES, LANES), 1)
    same = jnp.where((wide.T == wide) & (rows_iota < lane_iota), 1.0, 0.0)
    rank = jnp.sum(same, axis=0, keepdims=True)
    here = rows_iota.astype(jnp.float32) == wide
    for r in range(CAP):
        onehot = jnp.where(here & (rank == float(r)), 1.0, 0.0).astype(jnp.bfloat16)
        permute[pl.ds(r * LANES, LANES), pl.ds(0, LANES)] = onehot
        permute[pl.ds(r * LANES, LANES), pl.ds(LANES, LANES)] = onehot

    counts = counts_ref[...]
    for qb in range(NQB):
        weff[pl.ds(8 * qb, 8), :] = jnp.where(
            counts > qb, weights_ref[pl.ds(8 * qb, 8), :], 0.0
        )
    lame, shear = lame_ref[...], shear_ref[...]
    kmat[pl.ds(0, 8), :] = jnp.zeros((8, LANES), jnp.float32)
    kmat[pl.ds(0, 1), :] = slot_ref[...].astype(jnp.float32) + 1.0
    kmat[pl.ds(NWORDS, WORDS - NWORDS), :] = jnp.zeros((WORDS - NWORDS, LANES), jnp.float32)

    loads[-1].wait()

    def moments(a):
        gw = [
            [gbuf[3 * a + i, pl.ds(8 * qb, 8), :] * weff[pl.ds(8 * qb, 8), :] for qb in range(NQB)]
            for i in range(3)
        ]

        def one(b, carry):
            acc = [[None] * 3 for _ in range(3)]
            for qb in range(NQB):
                g = [gbuf[3 * b + j, pl.ds(8 * qb, 8), :] for j in range(3)]
                for i in range(3):
                    for j in range(3):
                        term = gw[i][qb] * g[j]
                        acc[i][j] = term if qb == 0 else acc[i][j] + term
            for i in range(3):
                for j in range(3):
                    partial[pl.ds((3 * i + j) * 8 * PITCH + b, 8, stride=PITCH), :] = acc[i][j]
            return carry

        lax.fori_loop(a, NF, one, 0)
        n = NF - a
        m = [[None] * 3 for _ in range(3)]
        for i in range(3):
            for j in range(3):
                base = (3 * i + j) * 8 * PITCH + a
                total = partial[pl.ds(base, n), :]
                for s in range(1, 8):
                    total = total + partial[pl.ds(base + s * PITCH, n), :]
                m[i][j] = total
        across = m[0][0] + m[1][1] + m[2][2]
        for i in range(3):
            for j in range(3):
                start, skip = SEGMENTS[a, i, j]
                if n == skip:
                    continue
                k = lame * m[i][j] + shear * (m[j][i] + across if i == j else m[j][i])
                kmat[pl.ds(start, n - skip), :] = k[skip:]

    def pack(c):
        for j in range((ROWS[c] + 1) // CAP):
            words = kmat[pl.ds(STARTS[c] + j * LANES, LANES), :]
            out = lax.dot_general(
                permute[...], split_high_low(words, 1), (((1,), (1,)), ((), ())),
                preferred_element_type=jnp.float32,
            )
            parts = [out[r * LANES:(r + 1) * LANES] for r in range(CAP)]
            if c == 0 and j == 0:
                parts[0] = jnp.where(lane_iota == 1, local_trace, parts[0])
            if CAP * (j + 1) > ROWS[c]:
                parts = [parts[0] + pltpu.roll(parts[1], HALF, 1)]
            for r, part in enumerate(parts):
                sendbuf[c, pl.ds(CAP * j + r, LANES, stride=8), :] = part
        own = pl.multiple_of(me * 8, 8)
        recvbuf[c, pl.ds(own, 8), :] = sendbuf[c, pl.ds(own, 8), :]

    def send(c):
        def to(peer_row, dc):
            peer = peer_row * ncol + cols_at[dc]
            pltpu.make_async_remote_copy(
                src_ref=sendbuf.at[c, pl.ds(pl.multiple_of(peer * 8, 8), ROWS[c]), :],
                dst_ref=recvbuf.at[c, pl.ds(pl.multiple_of(me * 8, 8), ROWS[c]), :],
                send_sem=send_sem.at[c],
                recv_sem=recv_sem.at[c],
                device_id=(peer_row, cols_at[dc]),
                device_id_type=MESH,
            ).start()

        def to_row(k, carry):
            peer_row = lax.rem(row + k, nrow)
            for dc in COL_ORDER:
                to(peer_row, dc)
            return carry

        lax.fori_loop(1, nrow, to_row, 0)
        for dc in range(1, ncol):
            to(row, dc)

    squares = [jnp.zeros((8, LANES), jnp.float32)] * NQB
    for m in range(NDOF):
        for qb in range(NQB):
            g = gbuf[m, pl.ds(8 * qb, 8), :]
            squares[qb] = squares[qb] + g * g
    weighted = sum(weff[pl.ds(8 * qb, 8), :] * squares[qb] for qb in range(NQB))
    local_trace = jnp.sum((lame + 4.0 * shear) * weighted)

    a = 0
    for c in range(len(ROWS)):
        need = min((STARTS + (NWORDS,))[c + 1], NWORDS)
        while a < NF and SEGMENTS[a, 0, 0][0] < need:
            moments(a)
            a += 1
        pack(c)
        if c == 0:
            pl.semaphore_wait(barrier, ndev - 1)
        send(c)

    def arrived(c):
        rows = (ndev - 1) * ROWS[c]
        pltpu.make_async_copy(
            recvbuf.at[c, pl.ds(0, rows), :], recvbuf.at[c, pl.ds(0, rows), :], recv_sem.at[c]
        ).wait()

    inverse = None
    pending = [key for key in SEGMENTS if NF - key[0] > SEGMENTS[key][1]]
    for c in range(len(ROWS)):
        arrived(c)
        for j in range((ROWS[c] + 1) // CAP):
            if CAP * (j + 1) > ROWS[c]:
                shared = recvbuf[c, pl.ds(CAP * j, LANES, stride=8), :]
                parts = [shared, pltpu.roll(shared, HALF, 1)]
            else:
                parts = [recvbuf[c, pl.ds(CAP * j + r, LANES, stride=8), :] for r in range(CAP)]
            words = jnp.concatenate(parts, axis=0)
            if c == 0 and j == 0:
                lanes = lax.broadcasted_iota(jnp.int32, (CAP * LANES, LANES), 1)
                hit = jnp.where(words[:, 0:1] - 1.0 == lanes.astype(jnp.float32), 1.0, 0.0)
                hit_t = jnp.concatenate([hit[0:LANES].T, hit[LANES:].T], axis=1)
                hit_t = hit_t.astype(jnp.bfloat16)
                place[...] = jnp.concatenate([hit_t, hit_t], axis=1)
                total = jnp.sum(parts[0][:, 1:2], axis=0, keepdims=True)
                inverse = jnp.broadcast_to(float(NDOF * LANES * ndev) / total, (8, LANES))
            out_t = jnp.dot(
                place[...], split_high_low(words, 0), preferred_element_type=jnp.float32
            )
            placed[pl.ds(STARTS[c] + j * LANES, LANES), :] = out_t.T
        while pending:
            a, i, j = pending[0]
            start, skip = SEGMENTS[a, i, j]
            n, b = NF - a - skip, a + skip
            if c < len(ROWS) - 1 and start + n > STARTS[c + 1]:
                break
            pending.pop(0)
            values = placed[pl.ds(start, n), :] * inverse[0:1]
            planes_ref[3 * a + i, pl.ds(3 * b + j, n, stride=3), :] = values
            for t in range(n):
                planes_ref[3 * (b + t) + j, pl.ds(3 * a + i, 1), :] = values[t:t + 1]

    for c in range(len(ROWS)):
        rows = (ndev - 1) * ROWS[c]
        pltpu.make_async_copy(
            sendbuf.at[c, pl.ds(0, rows), :], sendbuf.at[c, pl.ds(0, rows), :], send_sem.at[c]
        ).wait()


def shards(nrow, ncol, grads, weights, counts, lame_first, shear, dest_owner, dest_slot):
    count = grads.shape[3]
    vmem = pl.BlockSpec(memory_space=pltpu.VMEM)
    by_dof = jnp.transpose(grads, (1, 2, 0, 3)).reshape(NDOF, Q, count)
    return pl.pallas_call(
        functools.partial(exchange_kernel, nrow, ncol),
        out_shape=jax.ShapeDtypeStruct((NDOF, NDOF, LANES), jnp.float32),
        in_specs=[pl.BlockSpec(memory_space=pltpu.HBM)] * 7,
        out_specs=vmem,
        scratch_shapes=[
            pltpu.VMEM((NDOF, Q, LANES), jnp.float32),
            pltpu.VMEM((Q, LANES), jnp.float32),
            pltpu.VMEM((1, LANES), jnp.int32),
            pltpu.VMEM((1, LANES), jnp.float32),
            pltpu.VMEM((1, LANES), jnp.float32),
            pltpu.VMEM((1, LANES), jnp.int32),
            pltpu.VMEM((1, LANES), jnp.int32),
            pltpu.SemaphoreType.DMA((7,)),
            pltpu.VMEM((Q, LANES), jnp.float32),
            pltpu.VMEM((9 * 8 * PITCH + 24, LANES), jnp.float32),
            pltpu.VMEM((WORDS, LANES), jnp.float32),
            pltpu.VMEM((WORDS, LANES), jnp.float32),
            pltpu.VMEM((CAP * LANES, 2 * LANES), jnp.bfloat16),
            pltpu.VMEM((LANES, 2 * CAP * LANES), jnp.bfloat16),
            pltpu.VMEM((len(ROWS), LANES * 8 + 8, LANES), jnp.float32),
            pltpu.VMEM((len(ROWS), LANES * 8 + 8, LANES), jnp.float32),
            pltpu.SemaphoreType.DMA((len(ROWS),)),
            pltpu.SemaphoreType.DMA((len(ROWS),)),
        ],
        compiler_params=pltpu.CompilerParams(
            collective_id=0, has_side_effects=True, vmem_limit_bytes=24 << 20
        ),
    )(*(
        pltpu.with_memory_space_constraint(operand, pltpu.HBM)
        for operand in (
            by_dof, weights, counts.reshape(1, count), lame_first.reshape(1, count),
            shear.reshape(1, count), dest_owner.reshape(1, count), dest_slot.reshape(1, count),
        )
    ))


def solution(mesh):
    axes = ("row", "col")
    return jax.shard_map(
        functools.partial(shards, mesh.shape["row"], mesh.shape["col"]),
        mesh=mesh,
        in_specs=(
            P(None, None, None, axes),
            P(None, axes),
            P(axes),
            P(axes),
            P(axes),
            P(axes, None),
            P(axes),
        ),
        out_specs=P(None, None, axes),
        check_vma=False,
    )
```

```python
import functools

import jax
import jax.numpy as jnp
from jax import lax
from jax.experimental import pallas as pl
from jax.experimental.pallas import tpu as pltpu
from jax.sharding import PartitionSpec as P

NF = 20
NDOF = 60
Q = 64
NQB = 8
LANES = 128
CAP = 2
ROWS = (4, 6, 6, 6, 7)
STARTS = tuple(LANES * (sum(ROWS[:c]) // CAP) for c in range(len(ROWS)))
PITCH = 20
MESH = pl.DeviceIdType.MESH
COL_ORDER = (4, 5, 2, 3, 6, 7, 0, 1)


def segments():
    table, row = {}, 2
    for a in range(NF):
        for i in range(3):
            for j in range(3):
                skip = 1 if i > j else 0
                table[a, i, j] = (row, skip)
                row += NF - a - skip
    return table, row


SEGMENTS, NWORDS = segments()
WORDS = 15 * LANES
HALF = LANES // 2


def split_high_low(x, axis):
    high = x.astype(jnp.bfloat16)
    low = (x - high.astype(jnp.float32)).astype(jnp.bfloat16)
    return jnp.concatenate([high, low], axis=axis)


def exchange_kernel(
    nrow, ncol,
    grads_hbm, weights_hbm, counts_hbm, lame_hbm, shear_hbm, owner_hbm, slot_hbm,
    planes_ref,
    gbuf, weights_ref, counts_ref, lame_ref, shear_ref, owner_ref, slot_ref, load_sems, weff, partial, kmat, placed, permute, place, sendbuf, recvbuf, send_sem, recv_sem,
):
    row, col = lax.axis_index("row"), lax.axis_index("col")
    me = row * ncol + col
    ndev = nrow * ncol

    loads = [
        pltpu.make_async_copy(source, target, load_sems.at[k])
        for k, (source, target) in enumerate((
            (owner_hbm, owner_ref), (counts_hbm, counts_ref), (lame_hbm, lame_ref),
            (shear_hbm, shear_ref), (slot_hbm, slot_ref), (weights_hbm, weights_ref),
            (grads_hbm, gbuf),
        ))
    ]
    for load in loads:
        load.start()

    barrier = pltpu.get_barrier_semaphore()

    rows_at = [lax.rem(row + k, nrow) for k in range(nrow)]
    cols_at = [lax.rem(col + k, ncol) for k in range(ncol)]
    hops = (0, 1, 2, 1)
    order = sorted(
        ((dr, dc) for dr in range(nrow) for dc in range(ncol) if dr or dc),
        key=lambda o: -(hops[o[0] // 4] + hops[o[0] % 4] + hops[o[1] // 2]),
    )
    for dr, dc in order:
        pl.semaphore_signal(
            barrier, inc=1, device_id=(rows_at[dr], cols_at[dc]), device_id_type=MESH
        )

    for load in loads[:-1]:
        load.wait()

    owner = owner_ref[...].astype(jnp.float32)
    wide = jnp.broadcast_to(owner, (LANES, LANES))
    rows_iota = lax.broadcasted_iota(jnp.int32, (LANES, LANES), 0)
    lane_iota = lax.broadcasted_iota(jnp.int32, (LANES, LANES), 1)
    same = jnp.where((wide.T == wide) & (rows_iota < lane_iota), 1.0, 0.0)
    rank = jnp.sum(same, axis=0, keepdims=True)
    here = rows_iota.astype(jnp.float32) == wide
    for r in range(CAP):
        onehot = jnp.where(here & (rank == float(r)), 1.0, 0.0).astype(jnp.bfloat16)
        permute[pl.ds(r * LANES, LANES), pl.ds(0, LANES)] = onehot
        permute[pl.ds(r * LANES, LANES), pl.ds(LANES, LANES)] = onehot

    counts = counts_ref[...]
    for qb in range(NQB):
        weff[pl.ds(8 * qb, 8), :] = jnp.where(
            counts > qb, weights_ref[pl.ds(8 * qb, 8), :], 0.0
        )
    lame, shear = lame_ref[...], shear_ref[...]
    kmat[pl.ds(0, 8), :] = jnp.zeros((8, LANES), jnp.float32)
    kmat[pl.ds(0, 1), :] = slot_ref[...].astype(jnp.float32) + 1.0
    kmat[pl.ds(NWORDS, WORDS - NWORDS), :] = jnp.zeros((WORDS - NWORDS, LANES), jnp.float32)

    loads[-1].wait()

    def moments(a):
        gw = [
            [gbuf[3 * a + i, pl.ds(8 * qb, 8), :] * weff[pl.ds(8 * qb, 8), :] for qb in range(NQB)]
            for i in range(3)
        ]

        def one(b, carry):
            acc = [[None] * 3 for _ in range(3)]
            for qb in range(NQB):
                g = [gbuf[3 * b + j, pl.ds(8 * qb, 8), :] for j in range(3)]
                for i in range(3):
                    for j in range(3):
                        term = gw[i][qb] * g[j]
                        acc[i][j] = term if qb == 0 else acc[i][j] + term
            for i in range(3):
                for j in range(3):
                    partial[pl.ds((3 * i + j) * 8 * PITCH + b, 8, stride=PITCH), :] = acc[i][j]
            return carry

        lax.fori_loop(a, NF, one, 0)
        n = NF - a
        m = [[None] * 3 for _ in range(3)]
        for i in range(3):
            for j in range(3):
                base = (3 * i + j) * 8 * PITCH + a
                total = partial[pl.ds(base, n), :]
                for s in range(1, 8):
                    total = total + partial[pl.ds(base + s * PITCH, n), :]
                m[i][j] = total
        across = m[0][0] + m[1][1] + m[2][2]
        for i in range(3):
            for j in range(3):
                start, skip = SEGMENTS[a, i, j]
                if n == skip:
                    continue
                k = lame * m[i][j] + shear * (m[j][i] + across if i == j else m[j][i])
                kmat[pl.ds(start, n - skip), :] = k[skip:]

    def pack(c):
        for j in range((ROWS[c] + 1) // CAP):
            words = kmat[pl.ds(STARTS[c] + j * LANES, LANES), :]
            out = lax.dot_general(
                permute[...], split_high_low(words, 1), (((1,), (1,)), ((), ())),
                preferred_element_type=jnp.float32,
            )
            parts = [out[r * LANES:(r + 1) * LANES] for r in range(CAP)]
            if c == 0 and j == 0:
                parts[0] = jnp.where(lane_iota == 1, local_trace, parts[0])
            if CAP * (j + 1) > ROWS[c]:
                parts = [parts[0] + pltpu.roll(parts[1], HALF, 1)]
            for r, part in enumerate(parts):
                sendbuf[c, pl.ds(CAP * j + r, LANES, stride=8), :] = part
        own = pl.multiple_of(me * 8, 8)
        recvbuf[c, pl.ds(own, 8), :] = sendbuf[c, pl.ds(own, 8), :]

    def send(c):
        def to(peer_row, dc):
            peer = peer_row * ncol + cols_at[dc]
            pltpu.make_async_remote_copy(
                src_ref=sendbuf.at[c, pl.ds(pl.multiple_of(peer * 8, 8), ROWS[c]), :],
                dst_ref=recvbuf.at[c, pl.ds(pl.multiple_of(me * 8, 8), ROWS[c]), :],
                send_sem=send_sem.at[c],
                recv_sem=recv_sem.at[c],
                device_id=(peer_row, cols_at[dc]),
                device_id_type=MESH,
            ).start()

        def to_row(k, carry):
            peer_row = lax.rem(row + k, nrow)
            for dc in COL_ORDER:
                to(peer_row, dc)
            return carry

        lax.fori_loop(1, nrow, to_row, 0)
        for dc in range(1, ncol):
            to(row, dc)

    squares = [jnp.zeros((8, LANES), jnp.float32)] * NQB
    for m in range(NDOF):
        for qb in range(NQB):
            g = gbuf[m, pl.ds(8 * qb, 8), :]
            squares[qb] = squares[qb] + g * g
    weighted = sum(weff[pl.ds(8 * qb, 8), :] * squares[qb] for qb in range(NQB))
    local_trace = jnp.sum((lame + 4.0 * shear) * weighted)

    a = 0
    for c in range(len(ROWS)):
        need = min((STARTS + (NWORDS,))[c + 1], NWORDS)
        while a < NF and SEGMENTS[a, 0, 0][0] < need:
            moments(a)
            a += 1
        pack(c)
        if c == 0:
            pl.semaphore_wait(barrier, ndev - 1)
        send(c)

    def arrived(c):
        rows = (ndev - 1) * ROWS[c]
        pltpu.make_async_copy(
            recvbuf.at[c, pl.ds(0, rows), :], recvbuf.at[c, pl.ds(0, rows), :], recv_sem.at[c]
        ).wait()

    inverse = None
    pending = [key for key in SEGMENTS if NF - key[0] > SEGMENTS[key][1]]
    for c in range(len(ROWS)):
        arrived(c)
        for j in range((ROWS[c] + 1) // CAP):
            if CAP * (j + 1) > ROWS[c]:
                shared = recvbuf[c, pl.ds(CAP * j, LANES, stride=8), :]
                parts = [shared, pltpu.roll(shared, HALF, 1)]
            else:
                parts = [recvbuf[c, pl.ds(CAP * j + r, LANES, stride=8), :] for r in range(CAP)]
            words = jnp.concatenate(parts, axis=0)
            if c == 0 and j == 0:
                lanes = lax.broadcasted_iota(jnp.int32, (CAP * LANES, LANES), 1)
                hit = jnp.where(words[:, 0:1] - 1.0 == lanes.astype(jnp.float32), 1.0, 0.0)
                hit_t = jnp.concatenate([hit[0:LANES].T, hit[LANES:].T], axis=1)
                hit_t = hit_t.astype(jnp.bfloat16)
                place[...] = jnp.concatenate([hit_t, hit_t], axis=1)
                total = jnp.sum(parts[0][:, 1:2], axis=0, keepdims=True)
                inverse = jnp.broadcast_to(float(NDOF * LANES * ndev) / total, (8, LANES))
            out_t = jnp.dot(
                place[...], split_high_low(words, 0), preferred_element_type=jnp.float32
            )
            placed[pl.ds(STARTS[c] + j * LANES, LANES), :] = out_t.T
        while pending:
            a, i, j = pending[0]
            start, skip = SEGMENTS[a, i, j]
            n, b = NF - a - skip, a + skip
            if c < len(ROWS) - 1 and start + n > STARTS[c + 1]:
                break
            pending.pop(0)
            values = placed[pl.ds(start, n), :] * inverse[0:1]
            planes_ref[3 * a + i, pl.ds(3 * b + j, n, stride=3), :] = values
            for t in range(n):
                planes_ref[3 * (b + t) + j, pl.ds(3 * a + i, 1), :] = values[t:t + 1]

    for c in range(len(ROWS)):
        rows = (ndev - 1) * ROWS[c]
        pltpu.make_async_copy(
            sendbuf.at[c, pl.ds(0, rows), :], sendbuf.at[c, pl.ds(0, rows), :], send_sem.at[c]
        ).wait()


def shards(nrow, ncol, grads, weights, counts, lame_first, shear, dest_owner, dest_slot):
    count = grads.shape[3]
    vmem = pl.BlockSpec(memory_space=pltpu.VMEM)
    by_dof = jnp.transpose(grads, (1, 2, 0, 3)).reshape(NDOF, Q, count)
    return pl.pallas_call(
        functools.partial(exchange_kernel, nrow, ncol),
        out_shape=jax.ShapeDtypeStruct((NDOF, NDOF, LANES), jnp.float32),
        in_specs=[pl.BlockSpec(memory_space=pltpu.HBM)] * 7,
        out_specs=vmem,
        scratch_shapes=[
            pltpu.VMEM((NDOF, Q, LANES), jnp.float32),
            pltpu.VMEM((Q, LANES), jnp.float32),
            pltpu.VMEM((1, LANES), jnp.int32),
            pltpu.VMEM((1, LANES), jnp.float32),
            pltpu.VMEM((1, LANES), jnp.float32),
            pltpu.VMEM((1, LANES), jnp.int32),
            pltpu.VMEM((1, LANES), jnp.int32),
            pltpu.SemaphoreType.DMA((7,)),
            pltpu.VMEM((Q, LANES), jnp.float32),
            pltpu.VMEM((9 * 8 * PITCH + 24, LANES), jnp.float32),
            pltpu.VMEM((WORDS, LANES), jnp.float32),
            pltpu.VMEM((WORDS, LANES), jnp.float32),
            pltpu.VMEM((CAP * LANES, 2 * LANES), jnp.bfloat16),
            pltpu.VMEM((LANES, 2 * CAP * LANES), jnp.bfloat16),
            pltpu.VMEM((len(ROWS), LANES * 8 + 8, LANES), jnp.float32),
            pltpu.VMEM((len(ROWS), LANES * 8 + 8, LANES), jnp.float32),
            pltpu.SemaphoreType.DMA((len(ROWS),)),
            pltpu.SemaphoreType.DMA((len(ROWS),)),
        ],
        compiler_params=pltpu.CompilerParams(
            collective_id=0, has_side_effects=True, vmem_limit_bytes=24 << 20
        ),
    )(*(
        pltpu.with_memory_space_constraint(operand, pltpu.HBM)
        for operand in (
            by_dof, weights, counts.reshape(1, count), lame_first.reshape(1, count),
            shear.reshape(1, count), dest_owner.reshape(1, count), dest_slot.reshape(1, count),
        )
    ))


def solution(mesh):
    axes = ("row", "col")
    return jax.shard_map(
        functools.partial(shards, mesh.shape["row"], mesh.shape["col"]),
        mesh=mesh,
        in_specs=(
            P(None, None, None, axes),
            P(None, axes),
            P(axes),
            P(axes),
            P(axes),
            P(axes, None),
            P(axes),
        ),
        out_specs=P(None, None, axes),
        check_vma=False,
    )
```

```python
import functools

import jax
import jax.numpy as jnp
from jax import lax
from jax.experimental import pallas as pl
from jax.experimental.pallas import tpu as pltpu
from jax.sharding import PartitionSpec as P

NF = 20
NDOF = 60
Q = 64
NQB = 8
LANES = 128
CAP = 2
ROWS = (4, 6, 6, 8, 5)
STARTS = tuple(LANES * (sum(ROWS[:c]) // CAP) for c in range(len(ROWS)))
PITCH = 20
MESH = pl.DeviceIdType.MESH
COL_ORDER = (4, 5, 2, 3, 6, 7, 0, 1)


def segments():
    table, row = {}, 2
    for a in range(NF):
        for i in range(3):
            for j in range(3):
                skip = 1 if i > j else 0
                table[a, i, j] = (row, skip)
                row += NF - a - skip
    return table, row


SEGMENTS, NWORDS = segments()
WORDS = 15 * LANES
HALF = LANES // 2


def split_high_low(x, axis):
    high = x.astype(jnp.bfloat16)
    low = (x - high.astype(jnp.float32)).astype(jnp.bfloat16)
    return jnp.concatenate([high, low], axis=axis)


def exchange_kernel(
    nrow, ncol,
    grads_hbm, weights_hbm, counts_hbm, lame_hbm, shear_hbm, owner_hbm, slot_hbm,
    planes_ref,
    gbuf, weights_ref, counts_ref, lame_ref, shear_ref, owner_ref, slot_ref, load_sems, weff, partial, kmat, placed, permute, place, sendbuf, recvbuf, send_sem, recv_sem,
):
    row, col = lax.axis_index("row"), lax.axis_index("col")
    me = row * ncol + col
    ndev = nrow * ncol

    loads = [
        pltpu.make_async_copy(source, target, load_sems.at[k])
        for k, (source, target) in enumerate((
            (owner_hbm, owner_ref), (counts_hbm, counts_ref), (lame_hbm, lame_ref),
            (shear_hbm, shear_ref), (slot_hbm, slot_ref), (weights_hbm, weights_ref),
            (grads_hbm, gbuf),
        ))
    ]
    for load in loads:
        load.start()

    barrier = pltpu.get_barrier_semaphore()

    rows_at = [lax.rem(row + k, nrow) for k in range(nrow)]
    cols_at = [lax.rem(col + k, ncol) for k in range(ncol)]
    hops = (0, 1, 2, 1)
    order = sorted(
        ((dr, dc) for dr in range(nrow) for dc in range(ncol) if dr or dc),
        key=lambda o: -(hops[o[0] // 4] + hops[o[0] % 4] + hops[o[1] // 2]),
    )
    for dr, dc in order:
        pl.semaphore_signal(
            barrier, inc=1, device_id=(rows_at[dr], cols_at[dc]), device_id_type=MESH
        )

    for load in loads[:-1]:
        load.wait()

    owner = owner_ref[...].astype(jnp.float32)
    wide = jnp.broadcast_to(owner, (LANES, LANES))
    rows_iota = lax.broadcasted_iota(jnp.int32, (LANES, LANES), 0)
    lane_iota = lax.broadcasted_iota(jnp.int32, (LANES, LANES), 1)
    same = jnp.where((wide.T == wide) & (rows_iota < lane_iota), 1.0, 0.0)
    rank = jnp.sum(same, axis=0, keepdims=True)
    here = rows_iota.astype(jnp.float32) == wide
    for r in range(CAP):
        onehot = jnp.where(here & (rank == float(r)), 1.0, 0.0).astype(jnp.bfloat16)
        permute[pl.ds(r * LANES, LANES), pl.ds(0, LANES)] = onehot
        permute[pl.ds(r * LANES, LANES), pl.ds(LANES, LANES)] = onehot

    counts = counts_ref[...]
    for qb in range(NQB):
        weff[pl.ds(8 * qb, 8), :] = jnp.where(
            counts > qb, weights_ref[pl.ds(8 * qb, 8), :], 0.0
        )
    lame, shear = lame_ref[...], shear_ref[...]
    kmat[pl.ds(0, 8), :] = jnp.zeros((8, LANES), jnp.float32)
    kmat[pl.ds(0, 1), :] = slot_ref[...].astype(jnp.float32) + 1.0
    kmat[pl.ds(NWORDS, WORDS - NWORDS), :] = jnp.zeros((WORDS - NWORDS, LANES), jnp.float32)

    loads[-1].wait()

    def moments(a):
        gw = [
            [gbuf[3 * a + i, pl.ds(8 * qb, 8), :] * weff[pl.ds(8 * qb, 8), :] for qb in range(NQB)]
            for i in range(3)
        ]

        def one(b, carry):
            acc = [[None] * 3 for _ in range(3)]
            for qb in range(NQB):
                g = [gbuf[3 * b + j, pl.ds(8 * qb, 8), :] for j in range(3)]
                for i in range(3):
                    for j in range(3):
                        term = gw[i][qb] * g[j]
                        acc[i][j] = term if qb == 0 else acc[i][j] + term
            for i in range(3):
                for j in range(3):
                    partial[pl.ds((3 * i + j) * 8 * PITCH + b, 8, stride=PITCH), :] = acc[i][j]
            return carry

        lax.fori_loop(a, NF, one, 0)
        n = NF - a
        m = [[None] * 3 for _ in range(3)]
        for i in range(3):
            for j in range(3):
                base = (3 * i + j) * 8 * PITCH + a
                total = partial[pl.ds(base, n), :]
                for s in range(1, 8):
                    total = total + partial[pl.ds(base + s * PITCH, n), :]
                m[i][j] = total
        across = m[0][0] + m[1][1] + m[2][2]
        for i in range(3):
            for j in range(3):
                start, skip = SEGMENTS[a, i, j]
                if n == skip:
                    continue
                k = lame * m[i][j] + shear * (m[j][i] + across if i == j else m[j][i])
                kmat[pl.ds(start, n - skip), :] = k[skip:]

    def pack(c):
        for j in range((ROWS[c] + 1) // CAP):
            words = kmat[pl.ds(STARTS[c] + j * LANES, LANES), :]
            out = lax.dot_general(
                permute[...], split_high_low(words, 1), (((1,), (1,)), ((), ())),
                preferred_element_type=jnp.float32,
            )
            parts = [out[r * LANES:(r + 1) * LANES] for r in range(CAP)]
            if c == 0 and j == 0:
                parts[0] = jnp.where(lane_iota == 1, local_trace, parts[0])
            if CAP * (j + 1) > ROWS[c]:
                parts = [parts[0] + pltpu.roll(parts[1], HALF, 1)]
            for r, part in enumerate(parts):
                sendbuf[c, pl.ds(CAP * j + r, LANES, stride=8), :] = part
        own = pl.multiple_of(me * 8, 8)
        recvbuf[c, pl.ds(own, 8), :] = sendbuf[c, pl.ds(own, 8), :]

    def send(c):
        def to(peer_row, dc):
            peer = peer_row * ncol + cols_at[dc]
            pltpu.make_async_remote_copy(
                src_ref=sendbuf.at[c, pl.ds(pl.multiple_of(peer * 8, 8), ROWS[c]), :],
                dst_ref=recvbuf.at[c, pl.ds(pl.multiple_of(me * 8, 8), ROWS[c]), :],
                send_sem=send_sem.at[c],
                recv_sem=recv_sem.at[c],
                device_id=(peer_row, cols_at[dc]),
                device_id_type=MESH,
            ).start()

        def to_row(k, carry):
            peer_row = lax.rem(row + k, nrow)
            for dc in COL_ORDER:
                to(peer_row, dc)
            return carry

        lax.fori_loop(1, nrow, to_row, 0)
        for dc in range(1, ncol):
            to(row, dc)

    squares = [jnp.zeros((8, LANES), jnp.float32)] * NQB
    for m in range(NDOF):
        for qb in range(NQB):
            g = gbuf[m, pl.ds(8 * qb, 8), :]
            squares[qb] = squares[qb] + g * g
    weighted = sum(weff[pl.ds(8 * qb, 8), :] * squares[qb] for qb in range(NQB))
    local_trace = jnp.sum((lame + 4.0 * shear) * weighted)

    a = 0
    for c in range(len(ROWS)):
        need = min((STARTS + (NWORDS,))[c + 1], NWORDS)
        while a < NF and SEGMENTS[a, 0, 0][0] < need:
            moments(a)
            a += 1
        pack(c)
        if c == 0:
            pl.semaphore_wait(barrier, ndev - 1)
        send(c)

    def arrived(c):
        rows = (ndev - 1) * ROWS[c]
        pltpu.make_async_copy(
            recvbuf.at[c, pl.ds(0, rows), :], recvbuf.at[c, pl.ds(0, rows), :], recv_sem.at[c]
        ).wait()

    inverse = None
    pending = [key for key in SEGMENTS if NF - key[0] > SEGMENTS[key][1]]
    for c in range(len(ROWS)):
        arrived(c)
        for j in range((ROWS[c] + 1) // CAP):
            if CAP * (j + 1) > ROWS[c]:
                shared = recvbuf[c, pl.ds(CAP * j, LANES, stride=8), :]
                parts = [shared, pltpu.roll(shared, HALF, 1)]
            else:
                parts = [recvbuf[c, pl.ds(CAP * j + r, LANES, stride=8), :] for r in range(CAP)]
            words = jnp.concatenate(parts, axis=0)
            if c == 0 and j == 0:
                lanes = lax.broadcasted_iota(jnp.int32, (CAP * LANES, LANES), 1)
                hit = jnp.where(words[:, 0:1] - 1.0 == lanes.astype(jnp.float32), 1.0, 0.0)
                hit_t = jnp.concatenate([hit[0:LANES].T, hit[LANES:].T], axis=1)
                hit_t = hit_t.astype(jnp.bfloat16)
                place[...] = jnp.concatenate([hit_t, hit_t], axis=1)
                total = jnp.sum(parts[0][:, 1:2], axis=0, keepdims=True)
                inverse = jnp.broadcast_to(float(NDOF * LANES * ndev) / total, (8, LANES))
            out_t = jnp.dot(
                place[...], split_high_low(words, 0), preferred_element_type=jnp.float32
            )
            placed[pl.ds(STARTS[c] + j * LANES, LANES), :] = out_t.T
        while pending:
            a, i, j = pending[0]
            start, skip = SEGMENTS[a, i, j]
            n, b = NF - a - skip, a + skip
            if c < len(ROWS) - 1 and start + n > STARTS[c + 1]:
                break
            pending.pop(0)
            values = placed[pl.ds(start, n), :] * inverse[0:1]
            planes_ref[3 * a + i, pl.ds(3 * b + j, n, stride=3), :] = values
            for t in range(n):
                planes_ref[3 * (b + t) + j, pl.ds(3 * a + i, 1), :] = values[t:t + 1]

    for c in range(len(ROWS)):
        rows = (ndev - 1) * ROWS[c]
        pltpu.make_async_copy(
            sendbuf.at[c, pl.ds(0, rows), :], sendbuf.at[c, pl.ds(0, rows), :], send_sem.at[c]
        ).wait()


def shards(nrow, ncol, grads, weights, counts, lame_first, shear, dest_owner, dest_slot):
    count = grads.shape[3]
    vmem = pl.BlockSpec(memory_space=pltpu.VMEM)
    by_dof = jnp.transpose(grads, (1, 2, 0, 3)).reshape(NDOF, Q, count)
    return pl.pallas_call(
        functools.partial(exchange_kernel, nrow, ncol),
        out_shape=jax.ShapeDtypeStruct((NDOF, NDOF, LANES), jnp.float32),
        in_specs=[pl.BlockSpec(memory_space=pltpu.HBM)] * 7,
        out_specs=vmem,
        scratch_shapes=[
            pltpu.VMEM((NDOF, Q, LANES), jnp.float32),
            pltpu.VMEM((Q, LANES), jnp.float32),
            pltpu.VMEM((1, LANES), jnp.int32),
            pltpu.VMEM((1, LANES), jnp.float32),
            pltpu.VMEM((1, LANES), jnp.float32),
            pltpu.VMEM((1, LANES), jnp.int32),
            pltpu.VMEM((1, LANES), jnp.int32),
            pltpu.SemaphoreType.DMA((7,)),
            pltpu.VMEM((Q, LANES), jnp.float32),
            pltpu.VMEM((9 * 8 * PITCH + 24, LANES), jnp.float32),
            pltpu.VMEM((WORDS, LANES), jnp.float32),
            pltpu.VMEM((WORDS, LANES), jnp.float32),
            pltpu.VMEM((CAP * LANES, 2 * LANES), jnp.bfloat16),
            pltpu.VMEM((LANES, 2 * CAP * LANES), jnp.bfloat16),
            pltpu.VMEM((len(ROWS), LANES * 8 + 8, LANES), jnp.float32),
            pltpu.VMEM((len(ROWS), LANES * 8 + 8, LANES), jnp.float32),
            pltpu.SemaphoreType.DMA((len(ROWS),)),
            pltpu.SemaphoreType.DMA((len(ROWS),)),
        ],
        compiler_params=pltpu.CompilerParams(
            collective_id=0, has_side_effects=True, vmem_limit_bytes=24 << 20
        ),
    )(*(
        pltpu.with_memory_space_constraint(operand, pltpu.HBM)
        for operand in (
            by_dof, weights, counts.reshape(1, count), lame_first.reshape(1, count),
            shear.reshape(1, count), dest_owner.reshape(1, count), dest_slot.reshape(1, count),
        )
    ))


def solution(mesh):
    axes = ("row", "col")
    return jax.shard_map(
        functools.partial(shards, mesh.shape["row"], mesh.shape["col"]),
        mesh=mesh,
        in_specs=(
            P(None, None, None, axes),
            P(None, axes),
            P(axes),
            P(axes),
            P(axes),
            P(axes, None),
            P(axes),
        ),
        out_specs=P(None, None, axes),
        check_vma=False,
    )
```
